128 devices in a mesh: row: 8 (over x, core), col: 16 (over z, y).
Axes of the slice: x: 4, y: 4, z: 4, core: 2. Of those that a mesh axis runs over, the one named last changes fastest.
Arguments:
- fact_keys: int32 [32768], P(('row', 'col')), may hold values from 0 to 524287, as said below
- dim_keys: int32 [524288], P(('row', 'col')), may hold values from 0 to 524287, as said below
- dim_payload: bfloat16 [524288, 256], P(('row', 'col')), may hold values from -6 to 6
Outputs:
- joined: bfloat16 [32768, 256], P(('row', 'col'))
The draws below stay inside these ranges and needn't reach their ends.
Inputs may be any that keep to these rules, and one draw needn't show every extreme that they name: `fact_keys`: each key names a row of dim_keys. Its partition is key // 65536, and within it the block (key % 65536) // 4096. Among the 256 keys of one device at most 64 lie in one partition, and at most 8 in one block of one partition; in every draw one partition, the same on all devices, receives exactly 64 keys from every device, and some block of it exactly 8 keys from every device. `dim_keys`: the 4096 dimension rows of index r of the row axis and index c of the col axis hold the keys r * 65536 + c * 4096 to r * 65536 + (c + 1) * 4096 - 1, each once, in no particular order.
All inputs are finite; a program needn't handle non-finite values.
Results may differ from the reference program's by a relative error of at most 0.001.
Values may be sent and summed in bfloat16 or wider, within the bound.
A program may use at most 64 MiB of HBM per device.

```python
import jax
import jax.numpy as jnp

W = 256
DIM_DEV = 4096
F_DEV = 256
DIM = 524288
N_ROW = 8
N_COL = 16


def draw_dim_keys(key, part):
    part_size = DIM_DEV * N_COL
    subkeys = jax.random.split(jax.random.fold_in(key, 11), N_ROW * N_COL)
    permuted = jax.vmap(lambda sub_key: jax.random.permutation(sub_key, DIM_DEV))(subkeys)
    device_index = jnp.arange(N_ROW * N_COL, dtype=jnp.int32)
    offsets = device_index // N_COL * part_size + device_index % N_COL * DIM_DEV
    return (permuted.astype(jnp.int32) + offsets[:, None]).reshape(-1).astype(jnp.int32)


def draw_fact_keys(key, part):
    most = 2 * F_DEV // N_ROW
    sub_most = max(2, 2 * (most // N_COL))
    part_size = DIM_DEV * N_COL
    base_key = jax.random.fold_in(key, 23)
    hottest = jax.random.randint(jax.random.fold_in(base_key, 1), (), 0, N_ROW).astype(jnp.int32)
    order_keys = jax.random.split(jax.random.fold_in(base_key, 3), N_ROW)
    block_order = jax.vmap(lambda sub_key: jax.random.permutation(sub_key, N_COL))(order_keys).astype(jnp.int32)

    def one_device(dev_key):
        first_key, second_key, third_key = jax.random.split(dev_key, 3)
        shuffled = jax.random.permutation(first_key, (N_ROW - 1) * most)[:F_DEV - most].astype(jnp.int32)
        others = shuffled // most
        others = others + (others >= hottest).astype(jnp.int32)
        buckets = jnp.concatenate([jnp.full((most,), 0, jnp.int32) + hottest, others])
        buckets = jax.random.permutation(second_key, buckets).astype(jnp.int32)
        member = (buckets[:, None] == jnp.arange(N_ROW, dtype=jnp.int32)[None, :]).astype(jnp.int32)
        ranking = jnp.sum(jnp.cumsum(member, 0) * member, 1) - 1
        blocks = block_order[buckets, ranking // sub_most]
        offsets = jax.random.randint(third_key, (F_DEV,), 0, DIM_DEV).astype(jnp.int32)
        return buckets * part_size + blocks * DIM_DEV + offsets
    dev_keys = jax.random.split(jax.random.fold_in(base_key, 2), N_ROW * N_COL)
    return jax.vmap(one_device)(dev_keys).reshape(-1).astype(jnp.int32)


def levels(key, extent, shards, low, high):
    loudness, own = 1.0, jax.random.fold_in(key, 6)
    for dim, parts in shards:
        heights = jnp.exp(jax.random.uniform(jax.random.fold_in(own, dim), (parts,), jnp.float32, low / len(shards), high / len(shards)))
        loudness = loudness * jnp.repeat(heights, extent[dim] // parts).reshape([-1 if axis == dim else 1 for axis in range(len(extent))])
    return loudness


def centred(rng, shape, deviation, bound, cuts=(), kind=jnp.bfloat16):
    values = jax.random.normal(rng, shape, jnp.float32) * deviation
    if len(cuts) > 0:
        values = levels(rng, shape, cuts, -0.22, 0.18) * values
    return jnp.clip(values, min=-bound, max=bound).astype(kind)


def setup_inputs(seed: int = 0) -> dict:
    arg_keys = jax.random.split(jax.random.key(seed), 4)
    return {
        "fact_keys": draw_fact_keys(jax.random.fold_in(arg_keys[3], 71), 0),
        "dim_keys": draw_dim_keys(jax.random.fold_in(arg_keys[3], 71), 0),
        "dim_payload": centred(arg_keys[2], (DIM, W), 1.0, 6.0, ((0, 128),)),
    }


def reference(fact_keys, dim_keys, dim_payload):
    position = jnp.zeros((DIM,), jnp.int32).at[dim_keys].set(jnp.arange(DIM, dtype=jnp.int32))
    return dim_payload[position[fact_keys].astype(jnp.int32)]
```

```python
import functools

import jax
import jax.numpy as jnp
from jax import lax
from jax.experimental import pallas as pl
from jax.experimental.pallas import tpu as pltpu
from jax.sharding import PartitionSpec as P

MESH = pl.DeviceIdType.MESH
SLOTS = 8
ROWS = 8
COLS = 16
DEVICES = ROWS * COLS
GROUP = 32
GROUPS = DEVICES // GROUP
BLOCK = 4096
FACTS = 256
WIDTH = 256
STEP = 512


def code_of(offset):
    value = (128 + (offset & 127)).astype(jnp.float32)
    high = offset >> 7
    for bit in range(5):
        value = jnp.where(((high >> bit) & 1) == 1, value * float(2 ** (2**bit)), value)
    return value


def kernel(
    fact_ref,
    dim_ref,
    payload_ref,
    out_ref,
    table,
    codes,
    ask,
    asked,
    answer,
    got,
    place,
    copy_sem,
    ask_send,
    ask_recv,
    ans_send,
    ans_recv,
):
    row = lax.axis_index("row")
    col = lax.axis_index("col")
    me = row * COLS + col
    plane = me // GROUP
    inner = me % GROUP

    def peer(group, step):
        other = ((plane + group) % GROUPS) * GROUP + (inner + step) % GROUP
        return other, (other // COLS, other % COLS)

    barrier = pltpu.get_barrier_semaphore()
    for group in range(GROUPS):

        def greet(step, carry):
            unused, where = peer(group, step)
            pl.semaphore_signal(barrier, inc=1, device_id=where, device_id_type=MESH)
            return carry

        lax.fori_loop(1 if group == 0 else 0, GROUP, greet, 0)

    load = pltpu.make_async_copy(payload_ref, table, copy_sem)
    load.start()

    keys = jnp.concatenate([fact_ref[0:1, :], fact_ref[1:2, :]], axis=1)
    owner = keys >> 12
    code = code_of(keys & (BLOCK - 1))
    member = lax.broadcasted_iota(jnp.int32, (DEVICES, FACTS), 0) == owner
    member16 = member.astype(jnp.float32).astype(jnp.bfloat16)
    before = (
        lax.broadcasted_iota(jnp.int32, (FACTS, FACTS), 0)
        < lax.broadcasted_iota(jnp.int32, (FACTS, FACTS), 1)
    )
    before16 = before.astype(jnp.float32).astype(jnp.bfloat16)
    counts = jnp.dot(member16, before16, preferred_element_type=jnp.float32)
    rank = jnp.sum(jnp.where(member, counts, 0.0), axis=0, keepdims=True)
    coded = jnp.where(member, code, 0.0).astype(jnp.bfloat16)
    ranked = (
        lax.broadcasted_iota(jnp.int32, (DEVICES, FACTS), 0).astype(jnp.float32) == rank
    )
    ranked16 = ranked.astype(jnp.float32).astype(jnp.bfloat16)
    requests = lax.dot_general(
        coded, ranked16, (((1,), (1,)), ((), ())), preferred_element_type=jnp.float32
    )
    ask[...] = requests.reshape(DEVICES, 1, DEVICES)

    pl.semaphore_wait(barrier, DEVICES - 1)

    for group in (2, 1, 3, 0):

        def request(step, carry):
            other, where = peer(group, step)
            pltpu.make_async_remote_copy(
                src_ref=ask.at[other],
                dst_ref=asked.at[me],
                send_sem=ask_send,
                recv_sem=ask_recv.at[(GROUPS - group) % GROUPS],
                device_id=where,
                device_id_type=MESH,
            ).start()
            return carry

        lax.fori_loop(1 if group == 0 else 0, GROUP, request, 0)

    asked[me] = ask[me]

    dim_code = code_of(dim_ref[...] & (BLOCK - 1))
    for part in range(BLOCK // 128):
        codes[:, part * 128 : (part + 1) * 128] = jnp.broadcast_to(
            dim_code[part : part + 1, :], (16, 128)
        ).astype(jnp.bfloat16)

    slot_row = owner.astype(jnp.float32) * SLOTS + rank
    same = (
        lax.broadcasted_iota(jnp.int32, (FACTS, FACTS), 0)
        == lax.broadcasted_iota(jnp.int32, (FACTS, FACTS), 1)
    )
    slot = jnp.sum(jnp.where(same, slot_row, 0.0), axis=1, keepdims=True)
    slot = jnp.broadcast_to(slot, (FACTS, 128))
    lane = lax.broadcasted_iota(jnp.int32, (FACTS, 128), 1).astype(jnp.float32)
    for part in range(DEVICES * SLOTS // 128):
        place[:, part * 128 : (part + 1) * 128] = (
            (slot == lane + float(part * 128)).astype(jnp.float32).astype(jnp.bfloat16)
        )

    load.wait()

    picked = lax.broadcasted_iota(
        jnp.int32, (GROUP, SLOTS, 128), 1
    ) == lax.broadcasted_iota(jnp.int32, (GROUP, SLOTS, 128), 2)
    ones = jnp.ones((128, 128), jnp.bfloat16)
    rows = GROUP * SLOTS
    for group in (0, 1, 3, 2):
        source = (plane + group) % GROUPS
        first = source * GROUP
        count = GROUP - 1 if group == 0 else GROUP
        arrived = asked.at[pl.ds(0, count)]
        pltpu.make_async_copy(arrived, arrived, ask_recv.at[group]).wait()
        block = asked[pl.ds(first, GROUP)]
        spread = jnp.where(picked, jnp.broadcast_to(block, (GROUP, SLOTS, 128)), 0.0)
        spread = spread.reshape(rows, 128).astype(jnp.bfloat16)
        query = jnp.dot(spread, ones, preferred_element_type=jnp.float32).astype(jnp.bfloat16)
        wide = jnp.concatenate([query] * (STEP // 128), axis=1)
        total = jnp.zeros((rows, WIDTH), jnp.float32)
        for part in range(BLOCK // STEP):
            code_row = codes[:, part * STEP : (part + 1) * STEP]
            hit = jnp.concatenate([code_row] * (rows // 16), axis=0) == wide
            hit = jnp.where(hit, jnp.bfloat16(1), jnp.bfloat16(0))
            total = total + jnp.dot(
                hit,
                table[part * STEP : (part + 1) * STEP, :],
                preferred_element_type=jnp.float32,
            )
        answer[pl.ds(first, GROUP)] = total.astype(jnp.bfloat16).reshape(GROUP, SLOTS, WIDTH)

        def reply(step, carry):
            other, where = peer(group, step)
            pltpu.make_async_remote_copy(
                src_ref=answer.at[other],
                dst_ref=got.at[me],
                send_sem=ans_send,
                recv_sem=ans_recv,
                device_id=where,
                device_id_type=MESH,
            ).start()
            return carry

        lax.fori_loop(1 if group == 0 else 0, GROUP, reply, 0)
        if group == 0:
            got[me] = answer[me]

    landed = got.at[pl.ds(0, DEVICES - 1)]
    pltpu.make_async_copy(landed, landed, ans_recv).wait()
    fetched = got[...].reshape(DEVICES * SLOTS, WIDTH)
    out_ref[...] = jnp.dot(
        place[...], fetched, preferred_element_type=jnp.float32
    ).astype(jnp.bfloat16)

    sent = ask.at[pl.ds(0, DEVICES - 1)]
    pltpu.make_async_copy(sent, sent, ask_send).wait()
    pltpu.make_async_copy(landed, landed, ans_send).wait()


def on_device(fact_keys, dim_keys, dim_payload):
    vmem = pl.BlockSpec(memory_space=pltpu.VMEM)
    return pl.pallas_call(
        kernel,
        out_shape=jax.ShapeDtypeStruct((FACTS, WIDTH), jnp.bfloat16),
        in_specs=[vmem, vmem, pl.BlockSpec(memory_space=pl.ANY)],
        out_specs=vmem,
        scratch_shapes=[
            pltpu.VMEM((BLOCK, WIDTH), jnp.bfloat16),
            pltpu.VMEM((16, BLOCK), jnp.bfloat16),
            pltpu.VMEM((DEVICES, 1, 128), jnp.float32),
            pltpu.VMEM((DEVICES, 1, 128), jnp.float32),
            pltpu.VMEM((DEVICES, SLOTS, WIDTH), jnp.bfloat16),
            pltpu.VMEM((DEVICES, SLOTS, WIDTH), jnp.bfloat16),
            pltpu.VMEM((FACTS, DEVICES * SLOTS), jnp.bfloat16),
            pltpu.SemaphoreType.DMA,
            pltpu.SemaphoreType.DMA,
            pltpu.SemaphoreType.DMA((GROUPS,)),
            pltpu.SemaphoreType.DMA,
            pltpu.SemaphoreType.DMA,
        ],
        compiler_params=pltpu.CompilerParams(collective_id=0, has_side_effects=True),
    )(fact_keys.reshape(2, 128), dim_keys.reshape(BLOCK // 128, 128), dim_payload)


def solution(mesh):
    return jax.shard_map(
        on_device,
        mesh=mesh,
        in_specs=(P(("row", "col")), P(("row", "col")), P(("row", "col"), None)),
        out_specs=P(("row", "col"), None),
        check_vma=False,
    )
```

```python
import jax
import jax.numpy as jnp
from jax import lax
from jax.experimental import pallas as pl
from jax.experimental.pallas import tpu as pltpu
from jax.sharding import PartitionSpec as P

MESH = pl.DeviceIdType.MESH
SLOTS = 8
ROWS = 8
COLS = 16
DEVICES = ROWS * COLS
PLANE = 4
BLOCK = 4096
FACTS = 256
WIDTH = 256
STEP = 512
ORDER = (0, 1, 3, 2)


def code_of(offset):
    high = offset >> 7
    scaled = ((128 + (offset & 127)) << (high & 15)).astype(jnp.float32)
    return scaled * jnp.where(high >= 16, 65536.0, 1.0)


def iota(shape, axis):
    return lax.broadcasted_iota(jnp.int32, shape, axis)


def bits(mask):
    return mask.astype(jnp.float32).astype(jnp.bfloat16)


def kernel(
    fact_hbm,
    dim_hbm,
    payload_ref,
    out_ref,
    facts,
    dims,
    table,
    codes,
    keys_at,
    tags,
    coded_at,
    answer,
    got,
    place,
    copy_sem,
    key_send,
    line_recv,
    plane_recv,
    ans_send,
    ans_recv,
):
    row = lax.axis_index("row")
    col = lax.axis_index("col")
    me = row * COLS + col
    depth = col // PLANE
    other_rows = [lax.rem(row + step, ROWS) for step in range(1, ROWS)]
    other_cols = {}
    for far in range(PLANE):
        layer = lax.rem(depth + far, PLANE)
        for near in range(PLANE):
            other_cols[far, near] = layer * PLANE + lax.rem(col + near, PLANE)

    load_facts = pltpu.make_async_copy(fact_hbm, facts, copy_sem.at[0])
    load_facts.start()
    barrier = pltpu.get_barrier_semaphore()
    for other in other_rows:
        pl.semaphore_signal(barrier, inc=1, device_id=(other, col), device_id_type=MESH)
    for far in range(PLANE):
        for near in range(PLANE):
            if far or near:
                pl.semaphore_signal(
                    barrier,
                    inc=1,
                    device_id=(row, other_cols[far, near]),
                    device_id_type=MESH,
                )
    load_dims = pltpu.make_async_copy(dim_hbm, dims, copy_sem.at[1])
    load_dims.start()
    load_table = pltpu.make_async_copy(payload_ref, table, copy_sem.at[2])
    load_table.start()
    load_facts.wait()

    keys = jnp.concatenate([facts[0:1, :], facts[1:2, :]], axis=1)
    owner = keys >> 12
    member = iota((DEVICES, FACTS), 0) == owner
    before = bits(iota((FACTS, FACTS), 0) < iota((FACTS, FACTS), 1))
    counts = jnp.dot(bits(member), before, preferred_element_type=jnp.float32)
    rank = jnp.sum(jnp.where(member, counts, 0.0), axis=0, keepdims=True)
    slot_row = owner * SLOTS + rank.astype(jnp.int32)
    packed = slot_row * BLOCK + (keys & (BLOCK - 1))
    mine = keys_at.at[col, row]
    mine[0:1, :] = packed[:, :128]
    mine[1:2, :] = packed[:, 128:]

    pl.semaphore_wait(barrier, ROWS + COLS - 2)

    for other in other_rows:
        pltpu.make_async_remote_copy(
            src_ref=mine,
            dst_ref=mine,
            send_sem=key_send.at[0],
            recv_sem=line_recv,
            device_id=(other, col),
            device_id_type=MESH,
        ).start()

    same = iota((FACTS, FACTS), 0) == iota((FACTS, FACTS), 1)
    slot = jnp.sum(
        jnp.where(same, slot_row.astype(jnp.float32), 0.0), axis=1, keepdims=True
    )
    slot = jnp.broadcast_to(slot, (FACTS, 128))
    lane = iota((FACTS, 128), 1).astype(jnp.float32)
    for part in range(DEVICES * SLOTS // 128):
        place[:, part * 128 : (part + 1) * 128] = bits(slot == lane + float(part * 128))

    line = keys_at.at[0, pl.ds(0, ROWS - 1)]
    pltpu.make_async_copy(line, line, line_recv).wait()

    for far in (2, 1, 3, 0):
        for near in (2, 1, 3, 0):
            if far or near:
                pltpu.make_async_remote_copy(
                    src_ref=keys_at.at[col],
                    dst_ref=keys_at.at[col],
                    send_sem=key_send.at[1],
                    recv_sem=plane_recv.at[(PLANE - far) % PLANE],
                    device_id=(row, other_cols[far, near]),
                    device_id_type=MESH,
                ).start()

    load_dims.wait()
    dim_code = code_of(dims[...] & (BLOCK - 1))
    for part in range(BLOCK // 128):
        codes[:, part * 128 : (part + 1) * 128] = jnp.broadcast_to(
            dim_code[part : part + 1, :], (16, 128)
        ).astype(jnp.bfloat16)
    load_table.wait()

    ones = jnp.ones((FACTS, 128), jnp.bfloat16)
    count = PLANE * ROWS
    rows = count * SLOTS
    wanted = me * SLOTS + iota((count, SLOTS, 128), 1)
    for far in ORDER:
        layer = lax.rem(depth + far, PLANE)
        arrived = keys_at.at[pl.ds(0, PLANE if far else PLANE - 1)]
        pltpu.make_async_copy(arrived, arrived, plane_recv.at[far]).wait()
        block = keys_at[pl.ds(layer * PLANE, PLANE)].reshape(count, 2, 128)
        tags[...] = block >> 12
        coded_at[...] = code_of(block & (BLOCK - 1))
        spread = []
        for half in range(2):
            tag = jnp.broadcast_to(tags[:, half : half + 1, :], (count, SLOTS, 128))
            code = jnp.broadcast_to(coded_at[:, half : half + 1, :], (count, SLOTS, 128))
            spread.append(
                jnp.where(tag == wanted, code, 0.0).reshape(rows, 128).astype(jnp.bfloat16)
            )
        query = jnp.dot(
            jnp.concatenate(spread, axis=1), ones, preferred_element_type=jnp.float32
        ).astype(jnp.bfloat16)
        wide = jnp.concatenate([query] * (STEP // 128), axis=1)
        total = jnp.zeros((rows, WIDTH), jnp.float32)
        for part in range(BLOCK // STEP):
            code_row = codes[:, part * STEP : (part + 1) * STEP]
            hit = jnp.concatenate([code_row] * (rows // 16), axis=0) == wide
            hit = jnp.where(hit, jnp.bfloat16(1), jnp.bfloat16(0))
            total = total + jnp.dot(
                hit,
                table[part * STEP : (part + 1) * STEP, :],
                preferred_element_type=jnp.float32,
            )
        answer[far * count : (far + 1) * count] = total.astype(jnp.bfloat16).reshape(
            count, SLOTS, WIDTH
        )
        for near in range(PLANE):
            there = layer * PLANE + near
            for other in range(ROWS):

                def reply(there=there, near=near, other=other, far=far):
                    pltpu.make_async_remote_copy(
                        src_ref=answer.at[far * count + near * ROWS + other],
                        dst_ref=got.at[me],
                        send_sem=ans_send,
                        recv_sem=ans_recv,
                        device_id=(other, there),
                        device_id_type=MESH,
                    ).start()

                if far:
                    reply()
                else:
                    pl.when(jnp.logical_or(other != row, there != col))(reply)

        if far == 0:
            got[me] = answer[lax.rem(col, PLANE) * ROWS + row]

    landed = got.at[pl.ds(0, DEVICES - 1)]
    pltpu.make_async_copy(landed, landed, ans_recv).wait()
    out_ref[...] = jnp.dot(
        place[...],
        got[...].reshape(DEVICES * SLOTS, WIDTH),
        preferred_element_type=jnp.float32,
    ).astype(jnp.bfloat16)

    pltpu.make_async_copy(line, line, key_send.at[0]).wait()
    sent = keys_at.at[pl.ds(0, COLS - 1)]
    pltpu.make_async_copy(sent, sent, key_send.at[1]).wait()
    pltpu.make_async_copy(landed, landed, ans_send).wait()


def on_device(fact_keys, dim_keys, dim_payload):
    whole = pl.BlockSpec(memory_space=pl.ANY)
    count = PLANE * ROWS
    return pl.pallas_call(
        kernel,
        out_shape=jax.ShapeDtypeStruct((FACTS, WIDTH), jnp.bfloat16),
        in_specs=[whole, whole, whole],
        out_specs=pl.BlockSpec(memory_space=pltpu.VMEM),
        scratch_shapes=[
            pltpu.VMEM((2, 128), jnp.int32),
            pltpu.VMEM((BLOCK // 128, 128), jnp.int32),
            pltpu.VMEM((BLOCK, WIDTH), jnp.bfloat16),
            pltpu.VMEM((16, BLOCK), jnp.bfloat16),
            pltpu.VMEM((COLS, ROWS, 2, 128), jnp.int32),
            pltpu.VMEM((count, 2, 128), jnp.int32),
            pltpu.VMEM((count, 2, 128), jnp.float32),
            pltpu.VMEM((DEVICES, SLOTS, WIDTH), jnp.bfloat16),
            pltpu.VMEM((DEVICES, SLOTS, WIDTH), jnp.bfloat16),
            pltpu.VMEM((FACTS, DEVICES * SLOTS), jnp.bfloat16),
            pltpu.SemaphoreType.DMA((3,)),
            pltpu.SemaphoreType.DMA((2,)),
            pltpu.SemaphoreType.DMA,
            pltpu.SemaphoreType.DMA((PLANE,)),
            pltpu.SemaphoreType.DMA,
            pltpu.SemaphoreType.DMA,
        ],
        compiler_params=pltpu.CompilerParams(collective_id=0, has_side_effects=True),
    )(fact_keys.reshape(2, 128), dim_keys.reshape(BLOCK // 128, 128), dim_payload)


def solution(mesh):
    return jax.shard_map(
        on_device,
        mesh=mesh,
        in_specs=(P(("row", "col")), P(("row", "col")), P(("row", "col"), None)),
        out_specs=P(("row", "col"), None),
        check_vma=False,
    )
```

```python
import jax
import jax.numpy as jnp
from jax import lax
from jax.experimental import pallas as pl
from jax.experimental.pallas import tpu as pltpu
from jax.sharding import PartitionSpec as P

MESH = pl.DeviceIdType.MESH
SLOTS = 8
ROWS = 8
COLS = 16
PLANES = 4
CORES = 2
DEVICES = ROWS * COLS
BLOCK = 4096
FACTS = 256
WIDTH = 256
STEP = 512
COUNT = CORES * COLS


def code_of(offset):
    high = offset >> 7
    scaled = ((128 + (offset & 127)) << (high & 15)).astype(jnp.float32)
    return scaled * jnp.where(high >= 16, 65536.0, 1.0)


def iota(shape, axis):
    return lax.broadcasted_iota(jnp.int32, shape, axis)


def bits(mask):
    return mask.astype(jnp.float32).astype(jnp.bfloat16)


def kernel(
    fact_hbm,
    dim_hbm,
    payload_ref,
    out_ref,
    facts,
    dims,
    table,
    codes,
    ask,
    asked,
    answer,
    got,
    place,
    copy_sem,
    key_send,
    plane_recv,
    line_recv,
    ans_send,
    ans_recv,
):
    row = lax.axis_index("row")
    col = lax.axis_index("col")
    me = row * COLS + col
    plane = row // CORES
    other_rows = [lax.rem(row + step, ROWS) for step in range(1, ROWS)]
    depth = col // 4
    other_cols = [
        lax.rem(depth + far, 4) * 4 + lax.rem(col + near, 4)
        for far in (2, 1, 3, 0)
        for near in (2, 1, 3, 0)
        if far or near
    ]

    load_facts = pltpu.make_async_copy(fact_hbm, facts, copy_sem.at[0])
    load_facts.start()
    barrier = pltpu.get_barrier_semaphore()
    for other in other_cols:
        pl.semaphore_signal(barrier, inc=1, device_id=(row, other), device_id_type=MESH)
    for other in other_rows:
        pl.semaphore_signal(barrier, inc=1, device_id=(other, col), device_id_type=MESH)
    load_dims = pltpu.make_async_copy(dim_hbm, dims, copy_sem.at[1])
    load_dims.start()
    load_table = pltpu.make_async_copy(payload_ref, table, copy_sem.at[2])
    load_table.start()
    load_facts.wait()

    keys = jnp.concatenate([facts[0:1, :], facts[1:2, :]], axis=1)
    owner = keys >> 12
    member = iota((DEVICES, FACTS), 0) == owner
    before = bits(iota((FACTS, FACTS), 0) < iota((FACTS, FACTS), 1))
    counts = jnp.dot(bits(member), before, preferred_element_type=jnp.float32)
    rank = jnp.sum(jnp.where(member, counts, 0.0), axis=0, keepdims=True).astype(jnp.int32)
    code = code_of(keys & (BLOCK - 1))
    by_col = jnp.where(iota((COLS, FACTS), 0) == (owner & (COLS - 1)), code, 0.0)
    by_slot = iota((128, FACTS), 0) == (owner >> 4) * SLOTS + rank
    requests = lax.dot_general(
        by_col.astype(jnp.bfloat16),
        bits(by_slot),
        (((1,), (1,)), ((), ())),
        preferred_element_type=jnp.float32,
    )
    ask[...] = requests.reshape(COLS, 1, 128)
    asked[row, col] = ask[col]

    pl.semaphore_wait(barrier, ROWS + COLS - 2)

    for other in other_cols:
        pltpu.make_async_remote_copy(
            src_ref=ask.at[other],
            dst_ref=asked.at[row, col],
            send_sem=key_send.at[0],
            recv_sem=plane_recv,
            device_id=(row, other),
            device_id_type=MESH,
        ).start()

    slot_row = owner * SLOTS + rank
    same = iota((FACTS, FACTS), 0) == iota((FACTS, FACTS), 1)
    slot = jnp.sum(
        jnp.where(same, slot_row.astype(jnp.float32), 0.0), axis=1, keepdims=True
    )
    slot = jnp.broadcast_to(slot, (FACTS, 128))
    lane = iota((FACTS, 128), 1).astype(jnp.float32)
    for part in range(DEVICES * SLOTS // 128):
        place[:, part * 128 : (part + 1) * 128] = bits(slot == lane + float(part * 128))
    load_dims.wait()
    dim_code = code_of(dims[...] & (BLOCK - 1))
    for part in range(BLOCK // 128):
        codes[:, part * 128 : (part + 1) * 128] = jnp.broadcast_to(
            dim_code[part : part + 1, :], (16, 128)
        ).astype(jnp.bfloat16)
    load_table.wait()

    sheet = asked.at[0, pl.ds(0, COLS - 1)]
    pltpu.make_async_copy(sheet, sheet, plane_recv).wait()

    for other in other_rows:
        pltpu.make_async_remote_copy(
            src_ref=asked.at[row],
            dst_ref=asked.at[row],
            send_sem=key_send.at[1],
            recv_sem=line_recv.at[row],
            device_id=(other, col),
            device_id_type=MESH,
        ).start()

    picked = iota((COUNT, SLOTS, 128), 2) == row * SLOTS + iota((COUNT, SLOTS, 128), 1)
    ones = jnp.ones((128, 128), jnp.bfloat16)
    rows = COUNT * SLOTS
    turns = [0, 1, 2, 3]

    def wait_for(turn):
        for core in range(CORES):
            source = turns[turn] * CORES + core

            def arrive(source=source):
                block = asked.at[0]
                pltpu.make_async_copy(block, block, line_recv.at[source]).wait()

            if True:
                pl.when(source != row)(arrive)
            else:
                arrive()

    def queries(turn):
        block = asked[pl.ds(turns[turn] * CORES, CORES)].reshape(COUNT, 1, 128)
        spread = jnp.where(picked, jnp.broadcast_to(block, (COUNT, SLOTS, 128)), 0.0)
        return jnp.dot(
            spread.reshape(rows, 128).astype(jnp.bfloat16),
            ones,
            preferred_element_type=jnp.float32,
        ).astype(jnp.bfloat16)

    def lookup(query):
        parts = []
        for half in range(2):
            wide = jnp.concatenate(
                [query[half * (rows // 2) : (half + 1) * (rows // 2)]] * (STEP // 128), axis=1
            )
            total = jnp.zeros((rows // 2, WIDTH), jnp.float32)
            for part in range(BLOCK // STEP):
                code_row = codes[:, part * STEP : (part + 1) * STEP]
                hit = jnp.concatenate([code_row] * (rows // 32), axis=0) == wide
                hit = jnp.where(hit, jnp.bfloat16(1), jnp.bfloat16(0))
                total = total + jnp.dot(
                    hit,
                    table[part * STEP : (part + 1) * STEP, :],
                    preferred_element_type=jnp.float32,
                )
            parts.append(total)
        return jnp.concatenate(parts, axis=0).astype(jnp.bfloat16)

    wait_for(0)
    ahead = queries(0)
    for turn in range(PLANES):
        query = ahead
        if turn + 1 < PLANES:
            wait_for(turn + 1)
            ahead = queries(turn + 1)
        else:
            pass
        answer[turn] = lookup(query).reshape(CORES, COLS, SLOTS, WIDTH)
        for there in range(COLS):
            for core in range(CORES):
                other = turns[turn] * CORES + core

                def reply(there=there, core=core, other=other, turn=turn):
                    pltpu.make_async_remote_copy(
                        src_ref=answer.at[turn, core, there],
                        dst_ref=got.at[me],
                        send_sem=ans_send,
                        recv_sem=ans_recv,
                        device_id=(other, there),
                        device_id_type=MESH,
                    ).start()

                if True:
                    pl.when(jnp.logical_or(other != row, there != col))(reply)
                else:
                    reply()

    got[me] = answer[plane, row % CORES, col]

    landed = got.at[pl.ds(0, DEVICES - 1)]
    pltpu.make_async_copy(landed, landed, ans_recv).wait()
    out_ref[...] = jnp.dot(
        place[...],
        got[...].reshape(DEVICES * SLOTS, WIDTH),
        preferred_element_type=jnp.float32,
    ).astype(jnp.bfloat16)

    pltpu.make_async_copy(sheet, sheet, key_send.at[0]).wait()
    sent = asked.at[pl.ds(0, ROWS - 1)]
    pltpu.make_async_copy(sent, sent, key_send.at[1]).wait()
    pltpu.make_async_copy(landed, landed, ans_send).wait()


def on_device(fact_keys, dim_keys, dim_payload):
    whole = pl.BlockSpec(memory_space=pl.ANY)
    return pl.pallas_call(
        kernel,
        out_shape=pltpu.VMEM((FACTS, WIDTH), jnp.bfloat16),
        in_specs=[whole, whole, whole],
        out_specs=pl.BlockSpec(memory_space=pltpu.VMEM),
        scratch_shapes=[
            pltpu.VMEM((2, 128), jnp.int32),
            pltpu.VMEM((BLOCK // 128, 128), jnp.int32),
            pltpu.VMEM((BLOCK, WIDTH), jnp.bfloat16),
            pltpu.VMEM((16, BLOCK), jnp.bfloat16),
            pltpu.VMEM((COLS, 1, 128), jnp.float32),
            pltpu.VMEM((ROWS, COLS, 1, 128), jnp.float32),
            pltpu.VMEM((PLANES, CORES, COLS, SLOTS, WIDTH), jnp.bfloat16),
            pltpu.VMEM((DEVICES, SLOTS, WIDTH), jnp.bfloat16),
            pltpu.VMEM((FACTS, DEVICES * SLOTS), jnp.bfloat16),
            pltpu.SemaphoreType.DMA((3,)),
            pltpu.SemaphoreType.DMA((2,)),
            pltpu.SemaphoreType.DMA,
            pltpu.SemaphoreType.DMA((ROWS,)),
            pltpu.SemaphoreType.DMA,
            pltpu.SemaphoreType.DMA,
        ],
        compiler_params=pltpu.CompilerParams(collective_id=0, has_side_effects=True),
    )(fact_keys.reshape(2, 128), dim_keys.reshape(BLOCK // 128, 128), dim_payload)


def solution(mesh):
    return jax.shard_map(
        on_device,
        mesh=mesh,
        in_specs=(P(("row", "col")), P(("row", "col")), P(("row", "col"), None)),
        out_specs=P(("row", "col"), None),
        check_vma=False,
    )
```

```python
import jax
import jax.numpy as jnp
from jax import lax
from jax.experimental import pallas as pl
from jax.experimental.pallas import tpu as pltpu
from jax.sharding import PartitionSpec as P

MESH = pl.DeviceIdType.MESH
SLOTS = 8
ROWS = 8
COLS = 16
SIDE = 4
PLANES = 4
CORES = 2
LINES = PLANES * CORES
SPOTS = SIDE * SIDE
DEVICES = ROWS * COLS
BLOCK = 4096
FACTS = 256
WIDTH = 256
STEP = 512
COUNT = CORES * SPOTS


def code_of(offset):
    high = offset >> 7
    scaled = ((128 + (offset & 127)) << (high & 15)).astype(jnp.float32)
    return scaled * jnp.where(high >= 16, 65536.0, 1.0)


def iota(shape, axis):
    return lax.broadcasted_iota(jnp.int32, shape, axis)


def bits(mask):
    return mask.astype(jnp.float32).astype(jnp.bfloat16)


def kernel(
    fact_hbm,
    dim_hbm,
    payload_ref,
    out_ref,
    facts,
    dims,
    table,
    codes,
    ask,
    asked,
    answer,
    got,
    place,
    copy_sem,
    key_send,
    key_recv,
    ans_send,
    ans_recv,
):
    row = lax.axis_index("row")
    col = lax.axis_index("col")
    me = row * COLS + col
    x, core = row // CORES, lax.rem(row, CORES)
    z, y = col // SIDE, lax.rem(col, SIDE)
    line, spot = z * CORES + core, x * SIDE + y
    plane = z

    def device(line, spot):
        return (
            spot // SIDE * CORES + line % CORES,
            line // CORES * SIDE + spot % SIDE,
        )

    load_facts = pltpu.make_async_copy(fact_hbm, facts, copy_sem.at[0])
    load_facts.start()
    barrier = pltpu.get_barrier_semaphore()
    for other in range(LINES):
        for there in range(SPOTS):

            def greet(other=other, there=there):
                pl.semaphore_signal(
                    barrier, inc=1, device_id=device(other, there), device_id_type=MESH
                )

            pl.when(jnp.logical_or(other != line, there != spot))(greet)
    load_dims = pltpu.make_async_copy(dim_hbm, dims, copy_sem.at[1])
    load_dims.start()
    load_table = pltpu.make_async_copy(payload_ref, table, copy_sem.at[2])
    load_table.start()
    load_facts.wait()

    keys = jnp.concatenate([facts[0:1, :], facts[1:2, :]], axis=1)
    owner = keys >> 12
    target = (((owner >> 2) & 3) * 2 + ((owner >> 4) & 1)) * SPOTS + (owner >> 5) * SIDE + (owner & 3)
    member = iota((DEVICES, FACTS), 0) == target
    before = bits(iota((FACTS, FACTS), 0) < iota((FACTS, FACTS), 1))
    counts = jnp.dot(bits(member), before, preferred_element_type=jnp.float32)
    rank = jnp.sum(jnp.where(member, counts, 0.0), axis=0, keepdims=True).astype(jnp.int32)
    code = code_of(keys & (BLOCK - 1))
    requests = lax.dot_general(
        jnp.where(member, code, 0.0).astype(jnp.bfloat16),
        bits(iota((128, FACTS), 0) == rank),
        (((1,), (1,)), ((), ())),
        preferred_element_type=jnp.float32,
    )
    ask[...] = requests.reshape(DEVICES, 1, 128)
    asked[line, spot] = ask[line * SPOTS + spot]

    pl.semaphore_wait(barrier, DEVICES - 1)

    for other in range(LINES):
        for there in range(SPOTS):

            def request(other=other, there=there):
                pltpu.make_async_remote_copy(
                    src_ref=ask.at[other * SPOTS + there],
                    dst_ref=asked.at[line, spot],
                    send_sem=key_send,
                    recv_sem=key_recv.at[plane],
                    device_id=device(other, there),
                    device_id_type=MESH,
                ).start()

            pl.when(jnp.logical_or(other != line, there != spot))(request)

    slot_row = owner * SLOTS + rank
    same = iota((FACTS, FACTS), 0) == iota((FACTS, FACTS), 1)
    slot = jnp.sum(
        jnp.where(same, slot_row.astype(jnp.float32), 0.0), axis=1, keepdims=True
    )
    slot = jnp.broadcast_to(slot, (FACTS, 128))
    lane = iota((FACTS, 128), 1).astype(jnp.float32)
    for part in range(DEVICES * SLOTS // 128):
        place[:, part * 128 : (part + 1) * 128] = bits(slot == lane + float(part * 128))
    load_dims.wait()
    dim_code = code_of(dims[...] & (BLOCK - 1))
    for part in range(BLOCK // 128):
        codes[:, part * 128 : (part + 1) * 128] = jnp.broadcast_to(
            dim_code[part : part + 1, :], (16, 128)
        ).astype(jnp.bfloat16)
    load_table.wait()

    picked = iota((COUNT, SLOTS, 128), 2) == iota((COUNT, SLOTS, 128), 1)
    ones = jnp.ones((128, 128), jnp.bfloat16)
    rows = COUNT * SLOTS
    turns = [0, 1, 2, 3]

    def wait_for(turn):
        def arrive(count):
            block = ask.at[pl.ds(0, count)]
            pltpu.make_async_copy(block, block, key_recv.at[turns[turn]]).wait()


        pl.when(plane == turns[turn])(lambda: arrive(COUNT - 1))
        pl.when(plane != turns[turn])(lambda: arrive(COUNT))

    def queries(turn):
        block = asked[pl.ds(turns[turn] * CORES, CORES)].reshape(COUNT, 1, 128)
        spread = jnp.where(picked, jnp.broadcast_to(block, (COUNT, SLOTS, 128)), 0.0)
        return jnp.dot(
            spread.reshape(rows, 128).astype(jnp.bfloat16),
            ones,
            preferred_element_type=jnp.float32,
        ).astype(jnp.bfloat16)

    def lookup(query):
        parts = []
        for half in range(2):
            wide = jnp.concatenate(
                [query[half * (rows // 2) : (half + 1) * (rows // 2)]] * (STEP // 128), axis=1
            )
            total = jnp.zeros((rows // 2, WIDTH), jnp.float32)
            for part in range(BLOCK // STEP):
                code_row = codes[:, part * STEP : (part + 1) * STEP]
                hit = jnp.concatenate([code_row] * (rows // 32), axis=0) == wide
                hit = jnp.where(hit, jnp.bfloat16(1), jnp.bfloat16(0))
                total = total + jnp.dot(
                    hit,
                    table[part * STEP : (part + 1) * STEP, :],
                    preferred_element_type=jnp.float32,
                )
            parts.append(total)
        return jnp.concatenate(parts, axis=0).astype(jnp.bfloat16)

    ahead = None
    for turn in range(PLANES):
        if ahead is None:
            wait_for(turn)
            query = queries(turn)
        else:
            query = ahead
        ahead = None
        if 1 <= turn < PLANES - 1:
            wait_for(turn + 1)
            ahead = queries(turn + 1)
        else:
            pass
        answer[turn] = lookup(query).reshape(CORES, SPOTS, SLOTS, WIDTH)
        for there, twin in [(t, c) for t in (0, 1, 4, 2, 5, 8, 3, 6, 9, 12, 7, 10, 13, 11, 14, 15) for c in range(CORES)]:
                other = turns[turn] * CORES + twin

                def reply(there=there, twin=twin, other=other, turn=turn):
                    pltpu.make_async_remote_copy(
                        src_ref=answer.at[turn, twin, there],
                        dst_ref=got.at[me],
                        send_sem=ans_send,
                        recv_sem=ans_recv,
                        device_id=device(other, there),
                        device_id_type=MESH,
                    ).start()

                if True:
                    pl.when(jnp.logical_or(other != line, there != spot))(reply)
                else:
                    reply()

    got[me] = answer[plane, core, spot]

    landed = got.at[pl.ds(0, DEVICES - 1)]
    pltpu.make_async_copy(landed, landed, ans_recv).wait()
    out_ref[...] = jnp.dot(
        place[...],
        got[...].reshape(DEVICES * SLOTS, WIDTH),
        preferred_element_type=jnp.float32,
    ).astype(jnp.bfloat16)

    sent = ask.at[pl.ds(0, DEVICES - 1)]
    pltpu.make_async_copy(sent, sent, key_send).wait()
    pltpu.make_async_copy(landed, landed, ans_send).wait()


def on_device(fact_keys, dim_keys, dim_payload):
    whole = pl.BlockSpec(memory_space=pl.ANY)
    return pl.pallas_call(
        kernel,
        out_shape=pltpu.VMEM((FACTS, WIDTH), jnp.bfloat16),
        in_specs=[whole, whole, whole],
        out_specs=pl.BlockSpec(memory_space=pltpu.VMEM),
        scratch_shapes=[
            pltpu.VMEM((2, 128), jnp.int32),
            pltpu.VMEM((BLOCK // 128, 128), jnp.int32),
            pltpu.VMEM((BLOCK, WIDTH), jnp.bfloat16),
            pltpu.VMEM((16, BLOCK), jnp.bfloat16),
            pltpu.VMEM((DEVICES, 1, 128), jnp.float32),
            pltpu.VMEM((LINES, SPOTS, 1, 128), jnp.float32),
            pltpu.VMEM((PLANES, CORES, SPOTS, SLOTS, WIDTH), jnp.bfloat16),
            pltpu.VMEM((DEVICES, SLOTS, WIDTH), jnp.bfloat16),
            pltpu.VMEM((FACTS, DEVICES * SLOTS), jnp.bfloat16),
            pltpu.SemaphoreType.DMA((3,)),
            pltpu.SemaphoreType.DMA,
            pltpu.SemaphoreType.DMA((PLANES,)),
            pltpu.SemaphoreType.DMA,
            pltpu.SemaphoreType.DMA,
        ],
        compiler_params=pltpu.CompilerParams(collective_id=0, has_side_effects=True),
    )(fact_keys.reshape(2, 128), dim_keys.reshape(BLOCK // 128, 128), dim_payload)


def solution(mesh):
    return jax.shard_map(
        on_device,
        mesh=mesh,
        in_specs=(P(("row", "col")), P(("row", "col")), P(("row", "col"), None)),
        out_specs=P(("row", "col"), None),
        check_vma=False,
    )
```

```python
import jax
import jax.numpy as jnp
from jax import lax
from jax.experimental import pallas as pl
from jax.experimental.pallas import tpu as pltpu
from jax.sharding import PartitionSpec as P

MESH = pl.DeviceIdType.MESH
SLOTS = 8
ROWS = 8
COLS = 16
SIDE = 4
PLANES = 4
CORES = 2
LINES = PLANES * CORES
SPOTS = SIDE * SIDE
DEVICES = ROWS * COLS
BLOCK = 4096
FACTS = 256
WIDTH = 256
STEP = 512
COUNT = CORES * SPOTS
EARLY = (0,)
FARS = (1, 2, 3, 0)
FIRST = tuple(
    (0,) + tuple((z + far) % PLANES for far in FARS if (z + far) % PLANES) for z in range(PLANES)
)
INNER = ((0, 1), (0, 0), (1, 1), (1, 0), (4, 1), (4, 0), (2, 1), (2, 0), (5, 1), (5, 0), (8, 1), (8, 0), (3, 1), (3, 0), (6, 1), (6, 0), (9, 1), (9, 0), (12, 1), (12, 0), (7, 1), (7, 0), (10, 1), (10, 0), (13, 1), (13, 0), (11, 1), (11, 0), (14, 1), (14, 0), (15, 1), (15, 0))


def code_of(offset):
    high = offset >> 7
    scaled = ((128 + (offset & 127)) << (high & 15)).astype(jnp.float32)
    return scaled * jnp.where(high >= 16, 65536.0, 1.0)


def iota(shape, axis):
    return lax.broadcasted_iota(jnp.int32, shape, axis)


def bits(mask):
    return mask.astype(jnp.float32).astype(jnp.bfloat16)


def kernel(
    fact_hbm,
    dim_hbm,
    payload_ref,
    out_ref,
    facts,
    dims,
    table,
    codes,
    ask,
    asked,
    answer,
    got,
    place,
    copy_sem,
    key_send,
    key_recv,
    ans_send,
    ans_recv,
):
    row = lax.axis_index("row")
    col = lax.axis_index("col")
    me = row * COLS + col
    x, core = row // CORES, lax.rem(row, CORES)
    z, y = col // SIDE, lax.rem(col, SIDE)
    line, spot = z * CORES + core, x * SIDE + y
    plane = z
    early = jnp.int32(0)
    for there in EARLY:
        early = jnp.where(spot == there, 1, early)

    def device(line, spot):
        return (
            spot // SIDE * CORES + line % CORES,
            line // CORES * SIDE + spot % SIDE,
        )

    load_facts = pltpu.make_async_copy(fact_hbm, facts, copy_sem.at[0])
    load_facts.start()
    barrier = pltpu.get_barrier_semaphore()
    for other in range(LINES):
        for there in range(SPOTS):

            def greet(other=other, there=there):
                pl.semaphore_signal(
                    barrier, inc=1, device_id=device(other, there), device_id_type=MESH
                )

            pl.when(jnp.logical_or(other != line, there != spot))(greet)
    load_dims = pltpu.make_async_copy(dim_hbm, dims, copy_sem.at[1])
    load_dims.start()
    load_table = pltpu.make_async_copy(payload_ref, table, copy_sem.at[2])
    load_table.start()
    load_facts.wait()

    keys = jnp.concatenate([facts[0:1, :], facts[1:2, :]], axis=1)
    owner = keys >> 12
    target = (((owner >> 2) & 3) * 2 + ((owner >> 4) & 1)) * SPOTS + (owner >> 5) * SIDE + (owner & 3)
    member = iota((DEVICES, FACTS), 0) == target
    before = bits(iota((FACTS, FACTS), 0) < iota((FACTS, FACTS), 1))
    counts = jnp.dot(bits(member), before, preferred_element_type=jnp.float32)
    rank = jnp.sum(jnp.where(member, counts, 0.0), axis=0, keepdims=True).astype(jnp.int32)
    code = code_of(keys & (BLOCK - 1))
    requests = lax.dot_general(
        jnp.where(member, code, 0.0).astype(jnp.bfloat16),
        bits(iota((128, FACTS), 0) == rank),
        (((1,), (1,)), ((), ())),
        preferred_element_type=jnp.float32,
    )
    ask[...] = requests.reshape(DEVICES, 1, 128)
    asked[line, spot] = ask[line * SPOTS + spot]

    pl.semaphore_wait(barrier, DEVICES - 1)

    for other in range(LINES):
        for there in range(SPOTS):

            def request(other=other, there=there):
                pltpu.make_async_remote_copy(
                    src_ref=ask.at[other * SPOTS + there],
                    dst_ref=asked.at[line, spot],
                    send_sem=key_send,
                    recv_sem=key_recv.at[plane + PLANES * early],
                    device_id=device(other, there),
                    device_id_type=MESH,
                ).start()

            pl.when(jnp.logical_or(other != line, there != spot))(request)

    slot_row = owner * SLOTS + rank
    same = iota((FACTS, FACTS), 0) == iota((FACTS, FACTS), 1)
    slot = jnp.sum(
        jnp.where(same, slot_row.astype(jnp.float32), 0.0), axis=1, keepdims=True
    )
    slot = jnp.broadcast_to(slot, (FACTS, 128))
    lane = iota((FACTS, 128), 1).astype(jnp.float32)
    for part in range(DEVICES * SLOTS // 128):
        place[:, part * 128 : (part + 1) * 128] = bits(slot == lane + float(part * 128))
    load_dims.wait()
    dim_code = code_of(dims[...] & (BLOCK - 1))
    for part in range(BLOCK // 128):
        codes[:, part * 128 : (part + 1) * 128] = jnp.broadcast_to(
            dim_code[part : part + 1, :], (16, 128)
        ).astype(jnp.bfloat16)
    load_table.wait()

    picked = iota((COUNT, SLOTS, 128), 2) == iota((COUNT, SLOTS, 128), 1)
    ones = jnp.ones((128, 128), jnp.bfloat16)
    rows = COUNT * SLOTS
    layers = [lax.rem(plane + far, PLANES) for far in FARS]

    firsts = []
    for turn in range(PLANES):
        first = jnp.int32(FIRST[0][turn])
        for other in range(1, PLANES):
            first = jnp.where(plane == other, FIRST[other][turn], first)
        firsts.append(first)

    def layer_of(turn, there):
        return firsts[turn] if there in EARLY else layers[turn]

    def wait_for(turn):
        def arrive(layer, group, count):
            block = ask.at[pl.ds(0, count)]
            pltpu.make_async_copy(block, block, key_recv.at[layer + PLANES * group]).wait()

        many = CORES * len(EARLY)
        here = jnp.logical_and(plane == firsts[turn], early == 1)
        if many:
            pl.when(here)(lambda: arrive(firsts[turn], 1, many - 1))
            pl.when(jnp.logical_not(here))(lambda: arrive(firsts[turn], 1, many))
        if FARS[turn]:
            arrive(layers[turn], 0, COUNT - many)
        else:
            pl.when(early == 0)(lambda: arrive(layers[turn], 0, COUNT - many - 1))
            pl.when(early == 1)(lambda: arrive(layers[turn], 0, COUNT - many))

    def queries(turn):
        block = jnp.concatenate(
            [
                asked[layer_of(turn, there) * CORES + twin, there : there + 1]
                for twin in range(CORES)
                for there in range(SPOTS)
            ],
            axis=0,
        )
        spread = jnp.where(picked, jnp.broadcast_to(block, (COUNT, SLOTS, 128)), 0.0)
        return jnp.dot(
            spread.reshape(rows, 128).astype(jnp.bfloat16),
            ones,
            preferred_element_type=jnp.float32,
        ).astype(jnp.bfloat16)

    def lookup(query):
        parts = []
        for half in range(2):
            wide = jnp.concatenate(
                [query[half * (rows // 2) : (half + 1) * (rows // 2)]] * (STEP // 128), axis=1
            )
            total = jnp.zeros((rows // 2, WIDTH), jnp.float32)
            for part in range(BLOCK // STEP):
                code_row = codes[:, part * STEP : (part + 1) * STEP]
                hit = jnp.concatenate([code_row] * (rows // 32), axis=0) == wide
                hit = jnp.where(hit, jnp.bfloat16(1), jnp.bfloat16(0))
                total = total + jnp.dot(
                    hit,
                    table[part * STEP : (part + 1) * STEP, :],
                    preferred_element_type=jnp.float32,
                )
            parts.append(total)
        return jnp.concatenate(parts, axis=0).astype(jnp.bfloat16)

    ahead = None
    for turn in range(PLANES):
        if ahead is None:
            wait_for(turn)
            query = queries(turn)
        else:
            query = ahead
        ahead = None
        if 1 <= turn < PLANES - 1:
            wait_for(turn + 1)
            ahead = queries(turn + 1)
        else:
            pass
        answer[turn] = lookup(query).reshape(CORES, SPOTS, SLOTS, WIDTH)
        for there, twin in INNER:
                other = layer_of(turn, there) * CORES + twin

                def reply(there=there, twin=twin, other=other, turn=turn):
                    pltpu.make_async_remote_copy(
                        src_ref=answer.at[turn, twin, there],
                        dst_ref=got.at[me],
                        send_sem=ans_send,
                        recv_sem=ans_recv,
                        device_id=device(other, there),
                        device_id_type=MESH,
                    ).start()

                if there in EARLY or not FARS[turn]:
                    pl.when(jnp.logical_or(other != line, there != spot))(reply)
                else:
                    reply()

    own = jnp.int32(FARS.index(0))
    for turn in range(PLANES):
        here = jnp.logical_and(early == 1, plane == firsts[turn])
        own = jnp.where(here, turn, own)
    got[me] = answer[own, core, spot]

    landed = got.at[pl.ds(0, DEVICES - 1)]
    pltpu.make_async_copy(landed, landed, ans_recv).wait()
    out_ref[...] = jnp.dot(
        place[...],
        got[...].reshape(DEVICES * SLOTS, WIDTH),
        preferred_element_type=jnp.float32,
    ).astype(jnp.bfloat16)

    sent = ask.at[pl.ds(0, DEVICES - 1)]
    pltpu.make_async_copy(sent, sent, key_send).wait()
    pltpu.make_async_copy(landed, landed, ans_send).wait()


def on_device(fact_keys, dim_keys, dim_payload):
    whole = pl.BlockSpec(memory_space=pl.ANY)
    return pl.pallas_call(
        kernel,
        out_shape=pltpu.VMEM((FACTS, WIDTH), jnp.bfloat16),
        in_specs=[whole, whole, whole],
        out_specs=pl.BlockSpec(memory_space=pltpu.VMEM),
        scratch_shapes=[
            pltpu.VMEM((2, 128), jnp.int32),
            pltpu.VMEM((BLOCK // 128, 128), jnp.int32),
            pltpu.VMEM((BLOCK, WIDTH), jnp.bfloat16),
            pltpu.VMEM((16, BLOCK), jnp.bfloat16),
            pltpu.VMEM((DEVICES, 1, 128), jnp.float32),
            pltpu.VMEM((LINES, SPOTS, 1, 128), jnp.float32),
            pltpu.VMEM((PLANES, CORES, SPOTS, SLOTS, WIDTH), jnp.bfloat16),
            pltpu.VMEM((DEVICES, SLOTS, WIDTH), jnp.bfloat16),
            pltpu.VMEM((FACTS, DEVICES * SLOTS), jnp.bfloat16),
            pltpu.SemaphoreType.DMA((3,)),
            pltpu.SemaphoreType.DMA,
            pltpu.SemaphoreType.DMA((2 * PLANES,)),
            pltpu.SemaphoreType.DMA,
            pltpu.SemaphoreType.DMA,
        ],
        compiler_params=pltpu.CompilerParams(collective_id=0, has_side_effects=True),
    )(fact_keys.reshape(2, 128), dim_keys.reshape(BLOCK // 128, 128), dim_payload)


def solution(mesh):
    return jax.shard_map(
        on_device,
        mesh=mesh,
        in_specs=(P(("row", "col")), P(("row", "col")), P(("row", "col"), None)),
        out_specs=P(("row", "col"), None),
        check_vma=False,
    )
```

```python
import jax
import jax.numpy as jnp
from jax import lax
from jax.experimental import pallas as pl
from jax.experimental.pallas import tpu as pltpu
from jax.sharding import PartitionSpec as P

MESH = pl.DeviceIdType.MESH
SLOTS = 8
ROWS = 8
COLS = 16
SIDE = 4
PLANES = 4
CORES = 2
LINES = PLANES * CORES
SPOTS = SIDE * SIDE
DEVICES = ROWS * COLS
BLOCK = 4096
FACTS = 256
WIDTH = 256
STEP = 512
COUNT = CORES * SPOTS
EARLY = (0,)
FARS = (1, 2, 3, 0)
LAST = (3, 1, 0, 2)
ASK_LINES = (5, 4, 7, 6, 3, 2, 1, 0)
ASK_SPOTS = (10, 6, 9, 11, 14, 2, 5, 7, 8, 13, 15, 1, 3, 4, 12, 0)
FIRST = tuple(
    (0,) + tuple((z + far) % PLANES for far in FARS if (z + far) % PLANES) for z in range(PLANES)
)
INNER = ((0, 1), (0, 0), (1, 1), (1, 0), (4, 1), (4, 0), (2, 1), (2, 0), (5, 1), (5, 0), (8, 1), (8, 0), (3, 1), (3, 0), (6, 1), (6, 0), (9, 1), (9, 0), (12, 1), (12, 0), (7, 1), (7, 0), (10, 1), (10, 0), (13, 1), (13, 0), (11, 1), (11, 0), (14, 1), (14, 0), (15, 1), (15, 0))


def code_of(offset):
    high = offset >> 7
    scaled = ((128 + (offset & 127)) << (high & 15)).astype(jnp.float32)
    return scaled * jnp.where(high >= 16, 65536.0, 1.0)


def iota(shape, axis):
    return lax.broadcasted_iota(jnp.int32, shape, axis)


def bits(mask):
    return mask.astype(jnp.float32).astype(jnp.bfloat16)


def kernel(
    fact_hbm,
    dim_hbm,
    payload_ref,
    out_ref,
    facts,
    dims,
    table,
    codes,
    ask,
    asked,
    answer,
    got,
    place,
    copy_sem,
    key_send,
    key_recv,
    ans_send,
    ans_recv,
):
    row = lax.axis_index("row")
    col = lax.axis_index("col")
    x, core = row // CORES, lax.rem(row, CORES)
    z, y = col // SIDE, lax.rem(col, SIDE)
    line, spot = z * CORES + core, x * SIDE + y
    mine = line * SPOTS + spot
    plane = z
    early = jnp.int32(0)
    for there in EARLY:
        early = jnp.where(spot == there, 1, early)

    def device(line, spot):
        return (
            spot // SIDE * CORES + line % CORES,
            line // CORES * SIDE + spot % SIDE,
        )

    load_facts = pltpu.make_async_copy(fact_hbm, facts, copy_sem.at[0])
    load_facts.start()
    barrier = pltpu.get_barrier_semaphore()
    for other in range(LINES):
        for there in range(SPOTS):

            def greet(other=other, there=there):
                pl.semaphore_signal(
                    barrier, inc=1, device_id=device(other, there), device_id_type=MESH
                )

            pl.when(jnp.logical_or(other != line, there != spot))(greet)
    load_dims = pltpu.make_async_copy(dim_hbm, dims, copy_sem.at[1])
    load_dims.start()
    load_table = pltpu.make_async_copy(payload_ref, table, copy_sem.at[2])
    load_table.start()
    load_facts.wait()

    keys = jnp.concatenate([facts[0:1, :], facts[1:2, :]], axis=1)
    owner = keys >> 12
    target = (((owner >> 2) & 3) * 2 + ((owner >> 4) & 1)) * SPOTS + (owner >> 5) * SIDE + (owner & 3)
    member = iota((DEVICES, FACTS), 0) == target
    before = bits(iota((FACTS, FACTS), 0) < iota((FACTS, FACTS), 1))
    counts = jnp.dot(bits(member), before, preferred_element_type=jnp.float32)
    rank = jnp.sum(jnp.where(member, counts, 0.0), axis=0, keepdims=True).astype(jnp.int32)
    code = code_of(keys & (BLOCK - 1))
    requests = lax.dot_general(
        jnp.where(member, code, 0.0).astype(jnp.bfloat16),
        bits(iota((128, FACTS), 0) == rank),
        (((1,), (1,)), ((), ())),
        preferred_element_type=jnp.float32,
    )
    ask[...] = requests.reshape(DEVICES, 1, 128)
    asked[line, spot] = ask[line * SPOTS + spot]

    pl.semaphore_wait(barrier, DEVICES - 1)

    for other in ASK_LINES:
        for there in ASK_SPOTS:

            def request(other=other, there=there):
                pltpu.make_async_remote_copy(
                    src_ref=ask.at[other * SPOTS + there],
                    dst_ref=asked.at[line, spot],
                    send_sem=key_send,
                    recv_sem=key_recv.at[plane + PLANES * early],
                    device_id=device(other, there),
                    device_id_type=MESH,
                ).start()

            pl.when(jnp.logical_or(other != line, there != spot))(request)

    slot_row = target * SLOTS + rank
    same = iota((FACTS, FACTS), 0) == iota((FACTS, FACTS), 1)
    slot = jnp.sum(
        jnp.where(same, slot_row.astype(jnp.float32), 0.0), axis=1, keepdims=True
    )
    slot = jnp.broadcast_to(slot, (FACTS, 128))
    lane = iota((FACTS, 128), 1).astype(jnp.float32)
    for part in range(DEVICES * SLOTS // 128):
        place[:, part * 128 : (part + 1) * 128] = bits(slot == lane + float(part * 128))
    load_dims.wait()
    dim_code = code_of(dims[...] & (BLOCK - 1))
    for part in range(BLOCK // 128):
        codes[:, part * 128 : (part + 1) * 128] = jnp.broadcast_to(
            dim_code[part : part + 1, :], (16, 128)
        ).astype(jnp.bfloat16)
    load_table.wait()

    picked = iota((COUNT, SLOTS, 128), 2) == iota((COUNT, SLOTS, 128), 1)
    ones = jnp.ones((128, 128), jnp.bfloat16)
    rows = COUNT * SLOTS
    layers = [lax.rem(plane + far, PLANES) for far in FARS]

    firsts = []
    for turn in range(PLANES):
        first = jnp.int32(FIRST[0][turn])
        for other in range(1, PLANES):
            first = jnp.where(plane == other, FIRST[other][turn], first)
        firsts.append(first)

    def layer_of(turn, there):
        return firsts[turn] if there in EARLY else layers[turn]

    def wait_for(turn):
        def arrive(layer, group, count):
            block = ask.at[pl.ds(0, count)]
            pltpu.make_async_copy(block, block, key_recv.at[layer + PLANES * group]).wait()

        many = CORES * len(EARLY)
        here = jnp.logical_and(plane == firsts[turn], early == 1)
        if many:
            pl.when(here)(lambda: arrive(firsts[turn], 1, many - 1))
            pl.when(jnp.logical_not(here))(lambda: arrive(firsts[turn], 1, many))
        if FARS[turn]:
            arrive(layers[turn], 0, COUNT - many)
        else:
            pl.when(early == 0)(lambda: arrive(layers[turn], 0, COUNT - many - 1))
            pl.when(early == 1)(lambda: arrive(layers[turn], 0, COUNT - many))

    def queries(turn):
        block = jnp.concatenate(
            [
                asked[layer_of(turn, there) * CORES + twin, there : there + 1]
                for twin in range(CORES)
                for there in range(SPOTS)
            ],
            axis=0,
        )
        spread = jnp.where(picked, jnp.broadcast_to(block, (COUNT, SLOTS, 128)), 0.0)
        return jnp.dot(
            spread.reshape(rows, 128).astype(jnp.bfloat16),
            ones,
            preferred_element_type=jnp.float32,
        ).astype(jnp.bfloat16)

    def lookup(query):
        parts = []
        for half in range(2):
            wide = jnp.concatenate(
                [query[half * (rows // 2) : (half + 1) * (rows // 2)]] * (STEP // 128), axis=1
            )
            total = jnp.zeros((rows // 2, WIDTH), jnp.float32)
            for part in range(BLOCK // STEP):
                code_row = codes[:, part * STEP : (part + 1) * STEP]
                hit = jnp.concatenate([code_row] * (rows // 32), axis=0) == wide
                hit = jnp.where(hit, jnp.bfloat16(1), jnp.bfloat16(0))
                total = total + jnp.dot(
                    hit,
                    table[part * STEP : (part + 1) * STEP, :],
                    preferred_element_type=jnp.float32,
                )
            parts.append(total)
        return jnp.concatenate(parts, axis=0).astype(jnp.bfloat16)

    ahead = None
    for turn in range(PLANES):
        if ahead is None:
            wait_for(turn)
            query = queries(turn)
        else:
            query = ahead
        ahead = None
        if 1 <= turn < PLANES - 1:
            wait_for(turn + 1)
            ahead = queries(turn + 1)
        else:
            pass
        answer[turn] = lookup(query).reshape(CORES, SPOTS, SLOTS, WIDTH)
        for there, twin in INNER:
                other = layer_of(turn, there) * CORES + twin

                def reply(there=there, twin=twin, other=other, turn=turn):
                    pltpu.make_async_remote_copy(
                        src_ref=answer.at[turn, twin, there],
                        dst_ref=got.at[mine],
                        send_sem=ans_send,
                        recv_sem=ans_recv.at[plane],
                        device_id=device(other, there),
                        device_id_type=MESH,
                    ).start()

                if there in EARLY or not FARS[turn]:
                    pl.when(jnp.logical_or(other != line, there != spot))(reply)
                else:
                    reply()

    own = jnp.int32(FARS.index(0))
    for turn in range(PLANES):
        here = jnp.logical_and(early == 1, plane == firsts[turn])
        own = jnp.where(here, turn, own)
    got[mine] = answer[own, core, spot]

    landed = got.at[pl.ds(0, DEVICES - 1)]
    total = [jnp.zeros((FACTS // 2, WIDTH), jnp.float32)] * 2
    for far in LAST:
        layer = lax.rem(plane + far, PLANES)
        block = got.at[pl.ds(0, COUNT if far else COUNT - 1)]
        pltpu.make_async_copy(block, block, ans_recv.at[layer]).wait()
        fetched = got[pl.ds(layer * COUNT, COUNT)].reshape(rows, WIDTH)
        spots = pl.ds(pl.multiple_of(layer * rows, rows), rows)
        for half in range(2):
            part = slice(half * (FACTS // 2), (half + 1) * (FACTS // 2))
            total[half] = total[half] + jnp.dot(
                place[part, spots], fetched, preferred_element_type=jnp.float32
            )
    for half in range(2):
        part = slice(half * (FACTS // 2), (half + 1) * (FACTS // 2))
        out_ref[part, :] = total[half].astype(jnp.bfloat16)

    sent = ask.at[pl.ds(0, DEVICES - 1)]
    pltpu.make_async_copy(sent, sent, key_send).wait()
    pltpu.make_async_copy(landed, landed, ans_send).wait()


def on_device(fact_keys, dim_keys, dim_payload):
    whole = pl.BlockSpec(memory_space=pl.ANY)
    return pl.pallas_call(
        kernel,
        out_shape=pltpu.VMEM((FACTS, WIDTH), jnp.bfloat16),
        in_specs=[whole, whole, whole],
        out_specs=pl.BlockSpec(memory_space=pltpu.VMEM),
        scratch_shapes=[
            pltpu.VMEM((2, 128), jnp.int32),
            pltpu.VMEM((BLOCK // 128, 128), jnp.int32),
            pltpu.VMEM((BLOCK, WIDTH), jnp.bfloat16),
            pltpu.VMEM((16, BLOCK), jnp.bfloat16),
            pltpu.VMEM((DEVICES, 1, 128), jnp.float32),
            pltpu.VMEM((LINES, SPOTS, 1, 128), jnp.float32),
            pltpu.VMEM((PLANES, CORES, SPOTS, SLOTS, WIDTH), jnp.bfloat16),
            pltpu.VMEM((DEVICES, SLOTS, WIDTH), jnp.bfloat16),
            pltpu.VMEM((FACTS, DEVICES * SLOTS), jnp.bfloat16),
            pltpu.SemaphoreType.DMA((3,)),
            pltpu.SemaphoreType.DMA,
            pltpu.SemaphoreType.DMA((2 * PLANES,)),
            pltpu.SemaphoreType.DMA,
            pltpu.SemaphoreType.DMA((PLANES,)),
        ],
        compiler_params=pltpu.CompilerParams(collective_id=0, has_side_effects=True),
    )(fact_keys.reshape(2, 128), dim_keys.reshape(BLOCK // 128, 128), dim_payload)


def solution(mesh):
    return jax.shard_map(
        on_device,
        mesh=mesh,
        in_specs=(P(("row", "col")), P(("row", "col")), P(("row", "col"), None)),
        out_specs=P(("row", "col"), None),
        check_vma=False,
    )
```

```python
import jax
import jax.numpy as jnp
from jax import lax
from jax.experimental import pallas as pl
from jax.experimental.pallas import tpu as pltpu
from jax.sharding import PartitionSpec as P

MESH = pl.DeviceIdType.MESH
SLOTS = 8
ROWS = 8
COLS = 16
SIDE = 4
PLANES = 4
CORES = 2
LINES = PLANES * CORES
SPOTS = SIDE * SIDE
DEVICES = ROWS * COLS
BLOCK = 4096
FACTS = 256
WIDTH = 256
STEP = 512
COUNT = CORES * SPOTS
EARLY = (0,)
FARS = (1, 2, 3, 0)
LAST = (3, 1, 0, 2)
ASK_LINES = (4, 5, 6, 7, 2, 3, 0, 1)
ASK_SPOTS = (10, 6, 9, 11, 14, 2, 5, 7, 8, 13, 15, 1, 3, 4, 12, 0)
FIRST = tuple(
    (0,) + tuple((z + far) % PLANES for far in FARS if (z + far) % PLANES) for z in range(PLANES)
)
INNER = ((0, 1), (0, 0), (1, 1), (1, 0), (4, 1), (4, 0), (2, 1), (2, 0), (5, 1), (5, 0), (8, 1), (8, 0), (3, 1), (3, 0), (6, 1), (6, 0), (9, 1), (9, 0), (12, 1), (12, 0), (7, 1), (7, 0), (10, 1), (10, 0), (13, 1), (13, 0), (11, 1), (11, 0), (14, 1), (14, 0), (15, 1), (15, 0))


def code_of(offset):
    high = offset >> 7
    scaled = ((128 + (offset & 127)) << (high & 15)).astype(jnp.float32)
    return scaled * jnp.where(high >= 16, 65536.0, 1.0)


def iota(shape, axis):
    return lax.broadcasted_iota(jnp.int32, shape, axis)


def bits(mask):
    return mask.astype(jnp.float32).astype(jnp.bfloat16)


def kernel(
    fact_hbm,
    dim_hbm,
    payload_ref,
    out_ref,
    facts,
    dims,
    table,
    codes,
    ask,
    asked,
    answer,
    got,
    place,
    copy_sem,
    key_send,
    key_recv,
    ans_send,
    ans_recv,
):
    row = lax.axis_index("row")
    col = lax.axis_index("col")
    x, core = row // CORES, lax.rem(row, CORES)
    z, y = col // SIDE, lax.rem(col, SIDE)
    line, spot = z * CORES + core, x * SIDE + y
    mine = line * SPOTS + spot
    plane = z
    early = jnp.int32(0)
    for there in EARLY:
        early = jnp.where(spot == there, 1, early)

    def device(line, spot):
        return (
            spot // SIDE * CORES + line % CORES,
            line // CORES * SIDE + spot % SIDE,
        )

    load_facts = pltpu.make_async_copy(fact_hbm, facts, copy_sem.at[0])
    load_facts.start()
    barrier = pltpu.get_barrier_semaphore()
    for other in range(LINES):
        for there in range(SPOTS):

            def greet(other=other, there=there):
                pl.semaphore_signal(
                    barrier, inc=1, device_id=device(other, there), device_id_type=MESH
                )

            pl.when(jnp.logical_or(other != line, there != spot))(greet)
    load_dims = pltpu.make_async_copy(dim_hbm, dims, copy_sem.at[1])
    load_dims.start()
    load_table = pltpu.make_async_copy(payload_ref, table, copy_sem.at[2])
    load_table.start()
    load_facts.wait()

    keys = jnp.concatenate([facts[0:1, :], facts[1:2, :]], axis=1)
    owner = keys >> 12
    target = (((owner >> 2) & 3) * 2 + ((owner >> 4) & 1)) * SPOTS + (owner >> 5) * SIDE + (owner & 3)
    member = iota((DEVICES, FACTS), 0) == target
    before = bits(iota((FACTS, FACTS), 0) < iota((FACTS, FACTS), 1))
    counts = jnp.dot(bits(member), before, preferred_element_type=jnp.float32)
    rank = jnp.sum(jnp.where(member, counts, 0.0), axis=0, keepdims=True).astype(jnp.int32)
    code = code_of(keys & (BLOCK - 1))
    requests = lax.dot_general(
        jnp.where(member, code, 0.0).astype(jnp.bfloat16),
        bits(iota((128, FACTS), 0) == rank),
        (((1,), (1,)), ((), ())),
        preferred_element_type=jnp.float32,
    )
    ask[...] = requests.reshape(DEVICES, 1, 128)
    asked[line, spot] = ask[line * SPOTS + spot]

    pl.semaphore_wait(barrier, DEVICES - 1)

    for other in ASK_LINES:
        for there in ASK_SPOTS:

            def request(other=other, there=there):
                pltpu.make_async_remote_copy(
                    src_ref=ask.at[other * SPOTS + there],
                    dst_ref=asked.at[line, spot],
                    send_sem=key_send,
                    recv_sem=key_recv.at[plane + PLANES * early],
                    device_id=device(other, there),
                    device_id_type=MESH,
                ).start()

            pl.when(jnp.logical_or(other != line, there != spot))(request)

    slot_row = target * SLOTS + rank
    same = iota((FACTS, FACTS), 0) == iota((FACTS, FACTS), 1)
    slot = jnp.sum(
        jnp.where(same, slot_row.astype(jnp.float32), 0.0), axis=1, keepdims=True
    )
    slot = jnp.broadcast_to(slot, (FACTS, 128))
    lane = iota((FACTS, 128), 1).astype(jnp.float32)
    for part in range(DEVICES * SLOTS // 128):
        place[:, part * 128 : (part + 1) * 128] = bits(slot == lane + float(part * 128))
    load_dims.wait()
    dim_code = code_of(dims[...] & (BLOCK - 1))
    for part in range(BLOCK // 128):
        codes[:, part * 128 : (part + 1) * 128] = jnp.broadcast_to(
            dim_code[part : part + 1, :], (16, 128)
        ).astype(jnp.bfloat16)
    load_table.wait()

    picked = iota((COUNT, SLOTS, 128), 2) == iota((COUNT, SLOTS, 128), 1)
    ones = jnp.ones((128, 128), jnp.bfloat16)
    rows = COUNT * SLOTS
    layers = [lax.rem(plane + far, PLANES) for far in FARS]

    firsts = []
    for turn in range(PLANES):
        first = jnp.int32(FIRST[0][turn])
        for other in range(1, PLANES):
            first = jnp.where(plane == other, FIRST[other][turn], first)
        firsts.append(first)

    def layer_of(turn, there):
        return firsts[turn] if there in EARLY else layers[turn]

    def wait_for(turn):
        def arrive(layer, group, count):
            block = ask.at[pl.ds(0, count)]
            pltpu.make_async_copy(block, block, key_recv.at[layer + PLANES * group]).wait()

        many = CORES * len(EARLY)
        here = jnp.logical_and(plane == firsts[turn], early == 1)
        if many:
            pl.when(here)(lambda: arrive(firsts[turn], 1, many - 1))
            pl.when(jnp.logical_not(here))(lambda: arrive(firsts[turn], 1, many))
        if FARS[turn]:
            arrive(layers[turn], 0, COUNT - many)
        else:
            pl.when(early == 0)(lambda: arrive(layers[turn], 0, COUNT - many - 1))
            pl.when(early == 1)(lambda: arrive(layers[turn], 0, COUNT - many))

    def queries(turn):
        block = jnp.concatenate(
            [
                asked[layer_of(turn, there) * CORES + twin, there : there + 1]
                for twin in range(CORES)
                for there in range(SPOTS)
            ],
            axis=0,
        )
        spread = jnp.where(picked, jnp.broadcast_to(block, (COUNT, SLOTS, 128)), 0.0)
        return jnp.dot(
            spread.reshape(rows, 128).astype(jnp.bfloat16),
            ones,
            preferred_element_type=jnp.float32,
        ).astype(jnp.bfloat16)

    def lookup(query):
        parts = []
        for half in range(2):
            wide = jnp.concatenate(
                [query[half * (rows // 2) : (half + 1) * (rows // 2)]] * (STEP // 128), axis=1
            )
            total = jnp.zeros((rows // 2, WIDTH), jnp.float32)
            for part in range(BLOCK // STEP):
                code_row = codes[:, part * STEP : (part + 1) * STEP]
                hit = jnp.concatenate([code_row] * (rows // 32), axis=0) == wide
                hit = jnp.where(hit, jnp.bfloat16(1), jnp.bfloat16(0))
                total = total + jnp.dot(
                    hit,
                    table[part * STEP : (part + 1) * STEP, :],
                    preferred_element_type=jnp.float32,
                )
            parts.append(total)
        return jnp.concatenate(parts, axis=0).astype(jnp.bfloat16)

    ahead = None
    for turn in range(PLANES):
        if ahead is None:
            wait_for(turn)
            query = queries(turn)
        else:
            query = ahead
        ahead = None
        if 1 <= turn < PLANES - 1:
            wait_for(turn + 1)
            ahead = queries(turn + 1)
        else:
            pass
        answer[turn] = lookup(query).reshape(CORES, SPOTS, SLOTS, WIDTH)
        for there, twin in INNER:
                other = layer_of(turn, there) * CORES + twin

                def reply(there=there, twin=twin, other=other, turn=turn):
                    pltpu.make_async_remote_copy(
                        src_ref=answer.at[turn, twin, there],
                        dst_ref=got.at[mine],
                        send_sem=ans_send,
                        recv_sem=ans_recv.at[plane],
                        device_id=device(other, there),
                        device_id_type=MESH,
                    ).start()

                if there in EARLY or not FARS[turn]:
                    pl.when(jnp.logical_or(other != line, there != spot))(reply)
                else:
                    reply()

    own = jnp.int32(FARS.index(0))
    for turn in range(PLANES):
        here = jnp.logical_and(early == 1, plane == firsts[turn])
        own = jnp.where(here, turn, own)
    got[mine] = answer[own, core, spot]

    landed = got.at[pl.ds(0, DEVICES - 1)]
    total = [jnp.zeros((FACTS // 2, WIDTH), jnp.float32)] * 2
    for far in LAST:
        layer = lax.rem(plane + far, PLANES)
        block = got.at[pl.ds(0, COUNT if far else COUNT - 1)]
        pltpu.make_async_copy(block, block, ans_recv.at[layer]).wait()
        fetched = got[pl.ds(layer * COUNT, COUNT)].reshape(rows, WIDTH)
        spots = pl.ds(pl.multiple_of(layer * rows, rows), rows)
        for half in range(2):
            part = slice(half * (FACTS // 2), (half + 1) * (FACTS // 2))
            total[half] = total[half] + jnp.dot(
                place[part, spots], fetched, preferred_element_type=jnp.float32
            )
    for half in range(2):
        part = slice(half * (FACTS // 2), (half + 1) * (FACTS // 2))
        out_ref[part, :] = total[half].astype(jnp.bfloat16)

    sent = ask.at[pl.ds(0, DEVICES - 1)]
    pltpu.make_async_copy(sent, sent, key_send).wait()
    pltpu.make_async_copy(landed, landed, ans_send).wait()


def on_device(fact_keys, dim_keys, dim_payload):
    whole = pl.BlockSpec(memory_space=pl.ANY)
    return pl.pallas_call(
        kernel,
        out_shape=pltpu.VMEM((FACTS, WIDTH), jnp.bfloat16),
        in_specs=[whole, whole, whole],
        out_specs=pl.BlockSpec(memory_space=pltpu.VMEM),
        scratch_shapes=[
            pltpu.VMEM((2, 128), jnp.int32),
            pltpu.VMEM((BLOCK // 128, 128), jnp.int32),
            pltpu.VMEM((BLOCK, WIDTH), jnp.bfloat16),
            pltpu.VMEM((16, BLOCK), jnp.bfloat16),
            pltpu.VMEM((DEVICES, 1, 128), jnp.float32),
            pltpu.VMEM((LINES, SPOTS, 1, 128), jnp.float32),
            pltpu.VMEM((PLANES, CORES, SPOTS, SLOTS, WIDTH), jnp.bfloat16),
            pltpu.VMEM((DEVICES, SLOTS, WIDTH), jnp.bfloat16),
            pltpu.VMEM((FACTS, DEVICES * SLOTS), jnp.bfloat16),
            pltpu.SemaphoreType.DMA((3,)),
            pltpu.SemaphoreType.DMA,
            pltpu.SemaphoreType.DMA((2 * PLANES,)),
            pltpu.SemaphoreType.DMA,
            pltpu.SemaphoreType.DMA((PLANES,)),
        ],
        compiler_params=pltpu.CompilerParams(collective_id=0, has_side_effects=True),
    )(fact_keys.reshape(2, 128), dim_keys.reshape(BLOCK // 128, 128), dim_payload)


def solution(mesh):
    return jax.shard_map(
        on_device,
        mesh=mesh,
        in_specs=(P(("row", "col")), P(("row", "col")), P(("row", "col"), None)),
        out_specs=P(("row", "col"), None),
        check_vma=False,
    )
```

```python
import jax
import jax.numpy as jnp
from jax import lax
from jax.experimental import pallas as pl
from jax.experimental.pallas import tpu as pltpu
from jax.sharding import PartitionSpec as P

MESH = pl.DeviceIdType.MESH
SLOTS = 8
ROWS = 8
COLS = 16
SIDE = 4
PLANES = 4
CORES = 2
LINES = PLANES * CORES
SPOTS = SIDE * SIDE
DEVICES = ROWS * COLS
BLOCK = 4096
FACTS = 256
WIDTH = 256
STEP = 512
COUNT = CORES * SPOTS
EARLY = (0,)
FARS = (1, 2, 3, 0)
LAST = (3, 1, 0, 2)
ASK_LINES = (5, 4, 7, 6, 3, 2, 1, 0)
ASK_SPOTS = (10, 6, 9, 11, 14, 2, 5, 7, 8, 13, 15, 1, 3, 4, 12, 0)
FIRST = tuple(
    (0,) + tuple((z + far) % PLANES for far in FARS if (z + far) % PLANES) for z in range(PLANES)
)
INNER = ((0, 1), (0, 0), (1, 1), (1, 0), (4, 1), (4, 0), (2, 1), (2, 0), (5, 1), (5, 0), (8, 1), (8, 0), (3, 1), (3, 0), (6, 1), (6, 0), (9, 1), (9, 0), (12, 1), (12, 0), (7, 1), (7, 0), (10, 1), (10, 0), (13, 1), (13, 0), (11, 1), (11, 0), (14, 1), (14, 0), (15, 1), (15, 0))


def code_of(offset):
    high = offset >> 7
    scaled = ((128 + (offset & 127)) << (high & 15)).astype(jnp.float32)
    return scaled * jnp.where(high >= 16, 65536.0, 1.0)


def iota(shape, axis):
    return lax.broadcasted_iota(jnp.int32, shape, axis)


def bits(mask):
    return mask.astype(jnp.float32).astype(jnp.bfloat16)


def kernel(
    fact_hbm,
    dim_hbm,
    payload_ref,
    out_ref,
    facts,
    dims,
    table,
    codes,
    ask,
    asked,
    answer,
    got,
    place,
    copy_sem,
    key_send,
    key_recv,
    ans_send,
    ans_recv,
):
    row = lax.axis_index("row")
    col = lax.axis_index("col")
    x, core = row // CORES, lax.rem(row, CORES)
    z, y = col // SIDE, lax.rem(col, SIDE)
    line, spot = z * CORES + core, x * SIDE + y
    mine = line * SPOTS + spot
    plane = z
    early = jnp.int32(0)
    for there in EARLY:
        early = jnp.where(spot == there, 1, early)

    def device(line, spot):
        return (
            spot // SIDE * CORES + line % CORES,
            line // CORES * SIDE + spot % SIDE,
        )

    load_facts = pltpu.make_async_copy(fact_hbm, facts, copy_sem.at[0])
    load_facts.start()
    barrier = pltpu.get_barrier_semaphore()
    for other in (1, 0, 3, 2, 5, 4, 7, 6):
        for there in range(SPOTS):

            def greet(other=other, there=there):
                pl.semaphore_signal(
                    barrier, inc=1, device_id=device(other, there), device_id_type=MESH
                )

            pl.when(jnp.logical_or(other != line, there != spot))(greet)
    load_dims = pltpu.make_async_copy(dim_hbm, dims, copy_sem.at[1])
    load_dims.start()
    load_table = pltpu.make_async_copy(payload_ref, table, copy_sem.at[2])
    load_table.start()
    load_facts.wait()

    keys = jnp.concatenate([facts[0:1, :], facts[1:2, :]], axis=1)
    owner = keys >> 12
    target = (((owner >> 2) & 3) * 2 + ((owner >> 4) & 1)) * SPOTS + (owner >> 5) * SIDE + (owner & 3)
    member = iota((DEVICES, FACTS), 0) == target
    before = bits(iota((FACTS, FACTS), 0) < iota((FACTS, FACTS), 1))
    counts = jnp.dot(bits(member), before, preferred_element_type=jnp.float32)
    rank = jnp.sum(jnp.where(member, counts, 0.0), axis=0, keepdims=True).astype(jnp.int32)
    code = code_of(keys & (BLOCK - 1))
    requests = lax.dot_general(
        jnp.where(member, code, 0.0).astype(jnp.bfloat16),
        bits(iota((128, FACTS), 0) == rank),
        (((1,), (1,)), ((), ())),
        preferred_element_type=jnp.float32,
    )
    ask[...] = requests.reshape(DEVICES, 1, 128)
    asked[line, spot] = ask[line * SPOTS + spot]

    pl.semaphore_wait(barrier, DEVICES - 1)

    for other in ASK_LINES:
        for there in ASK_SPOTS:

            def request(other=other, there=there):
                pltpu.make_async_remote_copy(
                    src_ref=ask.at[other * SPOTS + there],
                    dst_ref=asked.at[line, spot],
                    send_sem=key_send,
                    recv_sem=key_recv.at[plane + PLANES * early],
                    device_id=device(other, there),
                    device_id_type=MESH,
                ).start()

            pl.when(jnp.logical_or(other != line, there != spot))(request)

    slot_row = target * SLOTS + rank
    same = iota((FACTS, FACTS), 0) == iota((FACTS, FACTS), 1)
    slot = jnp.sum(
        jnp.where(same, slot_row.astype(jnp.float32), 0.0), axis=1, keepdims=True
    )
    slot = jnp.broadcast_to(slot, (FACTS, 128))
    lane = iota((FACTS, 128), 1).astype(jnp.float32)
    for part in range(DEVICES * SLOTS // 128):
        place[:, part * 128 : (part + 1) * 128] = bits(slot == lane + float(part * 128))
    load_dims.wait()
    dim_code = code_of(dims[...] & (BLOCK - 1))
    for part in range(BLOCK // 128):
        codes[:, part * 128 : (part + 1) * 128] = jnp.broadcast_to(
            dim_code[part : part + 1, :], (16, 128)
        ).astype(jnp.bfloat16)
    load_table.wait()

    picked = iota((COUNT, SLOTS, 128), 2) == iota((COUNT, SLOTS, 128), 1)
    ones = jnp.ones((128, 128), jnp.bfloat16)
    rows = COUNT * SLOTS
    layers = [lax.rem(plane + far, PLANES) for far in FARS]

    firsts = []
    for turn in range(PLANES):
        first = jnp.int32(FIRST[0][turn])
        for other in range(1, PLANES):
            first = jnp.where(plane == other, FIRST[other][turn], first)
        firsts.append(first)

    def layer_of(turn, there):
        return firsts[turn] if there in EARLY else layers[turn]

    def wait_for(turn):
        def arrive(layer, group, count):
            block = ask.at[pl.ds(0, count)]
            pltpu.make_async_copy(block, block, key_recv.at[layer + PLANES * group]).wait()

        many = CORES * len(EARLY)
        here = jnp.logical_and(plane == firsts[turn], early == 1)
        if many:
            pl.when(here)(lambda: arrive(firsts[turn], 1, many - 1))
            pl.when(jnp.logical_not(here))(lambda: arrive(firsts[turn], 1, many))
        if FARS[turn]:
            arrive(layers[turn], 0, COUNT - many)
        else:
            pl.when(early == 0)(lambda: arrive(layers[turn], 0, COUNT - many - 1))
            pl.when(early == 1)(lambda: arrive(layers[turn], 0, COUNT - many))

    def queries(turn):
        block = jnp.concatenate(
            [
                asked[layer_of(turn, there) * CORES + twin, there : there + 1]
                for twin in range(CORES)
                for there in range(SPOTS)
            ],
            axis=0,
        )
        spread = jnp.where(picked, jnp.broadcast_to(block, (COUNT, SLOTS, 128)), 0.0)
        return jnp.dot(
            spread.reshape(rows, 128).astype(jnp.bfloat16),
            ones,
            preferred_element_type=jnp.float32,
        ).astype(jnp.bfloat16)

    def lookup(query):
        parts = []
        for half in range(2):
            wide = jnp.concatenate(
                [query[half * (rows // 2) : (half + 1) * (rows // 2)]] * (STEP // 128), axis=1
            )
            total = jnp.zeros((rows // 2, WIDTH), jnp.float32)
            for part in range(BLOCK // STEP):
                code_row = codes[:, part * STEP : (part + 1) * STEP]
                hit = jnp.concatenate([code_row] * (rows // 32), axis=0) == wide
                hit = jnp.where(hit, jnp.bfloat16(1), jnp.bfloat16(0))
                total = total + jnp.dot(
                    hit,
                    table[part * STEP : (part + 1) * STEP, :],
                    preferred_element_type=jnp.float32,
                )
            parts.append(total)
        return jnp.concatenate(parts, axis=0).astype(jnp.bfloat16)

    ahead = None
    for turn in range(PLANES):
        if ahead is None:
            wait_for(turn)
            query = queries(turn)
        else:
            query = ahead
        ahead = None
        if 1 <= turn < PLANES - 1:
            wait_for(turn + 1)
            ahead = queries(turn + 1)
        else:
            pass
        answer[turn] = lookup(query).reshape(CORES, SPOTS, SLOTS, WIDTH)
        for there, twin in INNER:
                other = layer_of(turn, there) * CORES + twin

                def reply(there=there, twin=twin, other=other, turn=turn):
                    pltpu.make_async_remote_copy(
                        src_ref=answer.at[turn, twin, there],
                        dst_ref=got.at[mine],
                        send_sem=ans_send,
                        recv_sem=ans_recv.at[plane],
                        device_id=device(other, there),
                        device_id_type=MESH,
                    ).start()

                if there in EARLY or not FARS[turn]:
                    pl.when(jnp.logical_or(other != line, there != spot))(reply)
                else:
                    reply()

    own = jnp.int32(FARS.index(0))
    for turn in range(PLANES):
        here = jnp.logical_and(early == 1, plane == firsts[turn])
        own = jnp.where(here, turn, own)
    got[mine] = answer[own, core, spot]

    landed = got.at[pl.ds(0, DEVICES - 1)]
    total = [jnp.zeros((FACTS // 2, WIDTH), jnp.float32)] * 2
    for far in LAST:
        layer = lax.rem(plane + far, PLANES)
        block = got.at[pl.ds(0, COUNT if far else COUNT - 1)]
        pltpu.make_async_copy(block, block, ans_recv.at[layer]).wait()
        fetched = got[pl.ds(layer * COUNT, COUNT)].reshape(rows, WIDTH)
        spots = pl.ds(pl.multiple_of(layer * rows, rows), rows)
        for half in range(2):
            part = slice(half * (FACTS // 2), (half + 1) * (FACTS // 2))
            total[half] = total[half] + jnp.dot(
                place[part, spots], fetched, preferred_element_type=jnp.float32
            )
    for half in range(2):
        part = slice(half * (FACTS // 2), (half + 1) * (FACTS // 2))
        out_ref[part, :] = total[half].astype(jnp.bfloat16)

    sent = ask.at[pl.ds(0, DEVICES - 1)]
    pltpu.make_async_copy(sent, sent, key_send).wait()
    pltpu.make_async_copy(landed, landed, ans_send).wait()


def on_device(fact_keys, dim_keys, dim_payload):
    whole = pl.BlockSpec(memory_space=pl.ANY)
    return pl.pallas_call(
        kernel,
        out_shape=pltpu.VMEM((FACTS, WIDTH), jnp.bfloat16),
        in_specs=[whole, whole, whole],
        out_specs=pl.BlockSpec(memory_space=pltpu.VMEM),
        scratch_shapes=[
            pltpu.VMEM((2, 128), jnp.int32),
            pltpu.VMEM((BLOCK // 128, 128), jnp.int32),
            pltpu.VMEM((BLOCK, WIDTH), jnp.bfloat16),
            pltpu.VMEM((16, BLOCK), jnp.bfloat16),
            pltpu.VMEM((DEVICES, 1, 128), jnp.float32),
            pltpu.VMEM((LINES, SPOTS, 1, 128), jnp.float32),
            pltpu.VMEM((PLANES, CORES, SPOTS, SLOTS, WIDTH), jnp.bfloat16),
            pltpu.VMEM((DEVICES, SLOTS, WIDTH), jnp.bfloat16),
            pltpu.VMEM((FACTS, DEVICES * SLOTS), jnp.bfloat16),
            pltpu.SemaphoreType.DMA((3,)),
            pltpu.SemaphoreType.DMA,
            pltpu.SemaphoreType.DMA((2 * PLANES,)),
            pltpu.SemaphoreType.DMA,
            pltpu.SemaphoreType.DMA((PLANES,)),
        ],
        compiler_params=pltpu.CompilerParams(collective_id=0, has_side_effects=True),
    )(fact_keys.reshape(2, 128), dim_keys.reshape(BLOCK // 128, 128), dim_payload)


def solution(mesh):
    return jax.shard_map(
        on_device,
        mesh=mesh,
        in_specs=(P(("row", "col")), P(("row", "col")), P(("row", "col"), None)),
        out_specs=P(("row", "col"), None),
        check_vma=False,
    )
```

```python
import jax
import jax.numpy as jnp
from jax import lax
from jax.experimental import pallas as pl
from jax.experimental.pallas import tpu as pltpu
from jax.sharding import PartitionSpec as P

MESH = pl.DeviceIdType.MESH
SLOTS = 8
ROWS = 8
COLS = 16
SIDE = 4
PLANES = 4
CORES = 2
LINES = PLANES * CORES
SPOTS = SIDE * SIDE
DEVICES = ROWS * COLS
BLOCK = 4096
FACTS = 256
WIDTH = 256
STEP = 512
COUNT = CORES * SPOTS
EARLY = (0,)
FARS = (1, 2, 3, 0)
LAST = (3, 0, 1, 2)
ASK_LINES = (5, 4, 7, 6, 3, 2, 1, 0)
ASK_SPOTS = (10, 6, 9, 11, 14, 2, 5, 7, 8, 13, 15, 1, 3, 4, 12, 0)
FIRST = tuple(
    (0,) + tuple((z + far) % PLANES for far in FARS if (z + far) % PLANES) for z in range(PLANES)
)
INNER = ((0, 1), (0, 0), (1, 1), (1, 0), (4, 1), (4, 0), (2, 1), (2, 0), (5, 1), (5, 0), (8, 1), (8, 0), (3, 1), (3, 0), (6, 1), (6, 0), (9, 1), (9, 0), (12, 1), (12, 0), (7, 1), (7, 0), (10, 1), (10, 0), (13, 1), (13, 0), (11, 1), (11, 0), (14, 1), (14, 0), (15, 1), (15, 0))


def code_of(offset):
    high = offset >> 7
    scaled = ((128 + (offset & 127)) << (high & 15)).astype(jnp.float32)
    return scaled * jnp.where(high >= 16, 65536.0, 1.0)


def iota(shape, axis):
    return lax.broadcasted_iota(jnp.int32, shape, axis)


def bits(mask):
    return mask.astype(jnp.float32).astype(jnp.bfloat16)


def kernel(
    fact_hbm,
    dim_hbm,
    payload_ref,
    out_ref,
    facts,
    dims,
    table,
    codes,
    ask,
    asked,
    answer,
    got,
    place,
    copy_sem,
    key_send,
    key_recv,
    ans_send,
    ans_recv,
):
    row = lax.axis_index("row")
    col = lax.axis_index("col")
    x, core = row // CORES, lax.rem(row, CORES)
    z, y = col // SIDE, lax.rem(col, SIDE)
    line, spot = z * CORES + core, x * SIDE + y
    mine = line * SPOTS + spot
    plane = z
    early = jnp.int32(0)
    for there in EARLY:
        early = jnp.where(spot == there, 1, early)

    def device(line, spot):
        return (
            spot // SIDE * CORES + line % CORES,
            line // CORES * SIDE + spot % SIDE,
        )

    load_facts = pltpu.make_async_copy(fact_hbm, facts, copy_sem.at[0])
    load_facts.start()
    barrier = pltpu.get_barrier_semaphore()
    for other in range(LINES):
        for there in range(SPOTS):

            def greet(other=other, there=there):
                pl.semaphore_signal(
                    barrier, inc=1, device_id=device(other, there), device_id_type=MESH
                )

            pl.when(jnp.logical_or(other != line, there != spot))(greet)
    load_dims = pltpu.make_async_copy(dim_hbm, dims, copy_sem.at[1])
    load_dims.start()
    load_table = pltpu.make_async_copy(payload_ref, table, copy_sem.at[2])
    load_table.start()
    load_facts.wait()

    keys = jnp.concatenate([facts[0:1, :], facts[1:2, :]], axis=1)
    owner = keys >> 12
    target = (((owner >> 2) & 3) * 2 + ((owner >> 4) & 1)) * SPOTS + (owner >> 5) * SIDE + (owner & 3)
    member = iota((DEVICES, FACTS), 0) == target
    before = bits(iota((FACTS, FACTS), 0) < iota((FACTS, FACTS), 1))
    counts = jnp.dot(bits(member), before, preferred_element_type=jnp.float32)
    rank = jnp.sum(jnp.where(member, counts, 0.0), axis=0, keepdims=True).astype(jnp.int32)
    code = code_of(keys & (BLOCK - 1))
    requests = lax.dot_general(
        jnp.where(member, code, 0.0).astype(jnp.bfloat16),
        bits(iota((128, FACTS), 0) == rank),
        (((1,), (1,)), ((), ())),
        preferred_element_type=jnp.float32,
    )
    ask[...] = requests.reshape(DEVICES, 1, 128)
    asked[line, spot] = ask[line * SPOTS + spot]

    pl.semaphore_wait(barrier, DEVICES - 1)

    for other in ASK_LINES:
        for there in ASK_SPOTS:

            def request(other=other, there=there):
                pltpu.make_async_remote_copy(
                    src_ref=ask.at[other * SPOTS + there],
                    dst_ref=asked.at[line, spot],
                    send_sem=key_send,
                    recv_sem=key_recv.at[plane + PLANES * early],
                    device_id=device(other, there),
                    device_id_type=MESH,
                ).start()

            pl.when(jnp.logical_or(other != line, there != spot))(request)

    slot_row = target * SLOTS + rank
    same = iota((FACTS, FACTS), 0) == iota((FACTS, FACTS), 1)
    slot = jnp.sum(
        jnp.where(same, slot_row.astype(jnp.float32), 0.0), axis=1, keepdims=True
    )
    slot = jnp.broadcast_to(slot, (FACTS, 128))
    lane = iota((FACTS, 128), 1).astype(jnp.float32)
    for part in range(DEVICES * SLOTS // 128):
        place[:, part * 128 : (part + 1) * 128] = bits(slot == lane + float(part * 128))
    load_dims.wait()
    dim_code = code_of(dims[...] & (BLOCK - 1))
    for part in range(BLOCK // 128):
        codes[:, part * 128 : (part + 1) * 128] = jnp.broadcast_to(
            dim_code[part : part + 1, :], (16, 128)
        ).astype(jnp.bfloat16)
    load_table.wait()

    picked = iota((COUNT, SLOTS, 128), 2) == iota((COUNT, SLOTS, 128), 1)
    ones = jnp.ones((128, 128), jnp.bfloat16)
    rows = COUNT * SLOTS
    layers = [lax.rem(plane + far, PLANES) for far in FARS]

    firsts = []
    for turn in range(PLANES):
        first = jnp.int32(FIRST[0][turn])
        for other in range(1, PLANES):
            first = jnp.where(plane == other, FIRST[other][turn], first)
        firsts.append(first)

    def layer_of(turn, there):
        return firsts[turn] if there in EARLY else layers[turn]

    def wait_for(turn):
        def arrive(layer, group, count):
            block = ask.at[pl.ds(0, count)]
            pltpu.make_async_copy(block, block, key_recv.at[layer + PLANES * group]).wait()

        many = CORES * len(EARLY)
        here = jnp.logical_and(plane == firsts[turn], early == 1)
        if many:
            pl.when(here)(lambda: arrive(firsts[turn], 1, many - 1))
            pl.when(jnp.logical_not(here))(lambda: arrive(firsts[turn], 1, many))
        if FARS[turn]:
            arrive(layers[turn], 0, COUNT - many)
        else:
            pl.when(early == 0)(lambda: arrive(layers[turn], 0, COUNT - many - 1))
            pl.when(early == 1)(lambda: arrive(layers[turn], 0, COUNT - many))

    def queries(turn):
        block = jnp.concatenate(
            [
                asked[layer_of(turn, there) * CORES + twin, there : there + 1]
                for twin in range(CORES)
                for there in range(SPOTS)
            ],
            axis=0,
        )
        spread = jnp.where(picked, jnp.broadcast_to(block, (COUNT, SLOTS, 128)), 0.0)
        return jnp.dot(
            spread.reshape(rows, 128).astype(jnp.bfloat16),
            ones,
            preferred_element_type=jnp.float32,
        ).astype(jnp.bfloat16)

    def lookup(query):
        parts = []
        for half in range(2):
            wide = jnp.concatenate(
                [query[half * (rows // 2) : (half + 1) * (rows // 2)]] * (STEP // 128), axis=1
            )
            total = jnp.zeros((rows // 2, WIDTH), jnp.float32)
            for part in range(BLOCK // STEP):
                code_row = codes[:, part * STEP : (part + 1) * STEP]
                hit = jnp.concatenate([code_row] * (rows // 32), axis=0) == wide
                hit = jnp.where(hit, jnp.bfloat16(1), jnp.bfloat16(0))
                total = total + jnp.dot(
                    hit,
                    table[part * STEP : (part + 1) * STEP, :],
                    preferred_element_type=jnp.float32,
                )
            parts.append(total)
        return jnp.concatenate(parts, axis=0).astype(jnp.bfloat16)

    ahead = None
    for turn in range(PLANES):
        if ahead is None:
            wait_for(turn)
            query = queries(turn)
        else:
            query = ahead
        ahead = None
        if 1 <= turn < PLANES - 1:
            wait_for(turn + 1)
            ahead = queries(turn + 1)
        else:
            pass
        answer[turn] = lookup(query).reshape(CORES, SPOTS, SLOTS, WIDTH)
        for there, twin in INNER:
                other = layer_of(turn, there) * CORES + twin

                def reply(there=there, twin=twin, other=other, turn=turn):
                    pltpu.make_async_remote_copy(
                        src_ref=answer.at[turn, twin, there],
                        dst_ref=got.at[mine],
                        send_sem=ans_send,
                        recv_sem=ans_recv.at[plane],
                        device_id=device(other, there),
                        device_id_type=MESH,
                    ).start()

                if there in EARLY or not FARS[turn]:
                    pl.when(jnp.logical_or(other != line, there != spot))(reply)
                else:
                    reply()

    own = jnp.int32(FARS.index(0))
    for turn in range(PLANES):
        here = jnp.logical_and(early == 1, plane == firsts[turn])
        own = jnp.where(here, turn, own)
    got[mine] = answer[own, core, spot]

    landed = got.at[pl.ds(0, DEVICES - 1)]
    total = [jnp.zeros((FACTS // 2, WIDTH), jnp.float32)] * 2
    for far in LAST:
        layer = lax.rem(plane + far, PLANES)
        block = got.at[pl.ds(0, COUNT if far else COUNT - 1)]
        pltpu.make_async_copy(block, block, ans_recv.at[layer]).wait()
        fetched = got[pl.ds(layer * COUNT, COUNT)].reshape(rows, WIDTH)
        spots = pl.ds(pl.multiple_of(layer * rows, rows), rows)
        for half in range(2):
            part = slice(half * (FACTS // 2), (half + 1) * (FACTS // 2))
            total[half] = total[half] + jnp.dot(
                place[part, spots], fetched, preferred_element_type=jnp.float32
            )
    for half in range(2):
        part = slice(half * (FACTS // 2), (half + 1) * (FACTS // 2))
        out_ref[part, :] = total[half].astype(jnp.bfloat16)

    sent = ask.at[pl.ds(0, DEVICES - 1)]
    pltpu.make_async_copy(sent, sent, key_send).wait()
    pltpu.make_async_copy(landed, landed, ans_send).wait()


def on_device(fact_keys, dim_keys, dim_payload):
    whole = pl.BlockSpec(memory_space=pl.ANY)
    return pl.pallas_call(
        kernel,
        out_shape=pltpu.VMEM((FACTS, WIDTH), jnp.bfloat16),
        in_specs=[whole, whole, whole],
        out_specs=pl.BlockSpec(memory_space=pltpu.VMEM),
        scratch_shapes=[
            pltpu.VMEM((2, 128), jnp.int32),
            pltpu.VMEM((BLOCK // 128, 128), jnp.int32),
            pltpu.VMEM((BLOCK, WIDTH), jnp.bfloat16),
            pltpu.VMEM((16, BLOCK), jnp.bfloat16),
            pltpu.VMEM((DEVICES, 1, 128), jnp.float32),
            pltpu.VMEM((LINES, SPOTS, 1, 128), jnp.float32),
            pltpu.VMEM((PLANES, CORES, SPOTS, SLOTS, WIDTH), jnp.bfloat16),
            pltpu.VMEM((DEVICES, SLOTS, WIDTH), jnp.bfloat16),
            pltpu.VMEM((FACTS, DEVICES * SLOTS), jnp.bfloat16),
            pltpu.SemaphoreType.DMA((3,)),
            pltpu.SemaphoreType.DMA,
            pltpu.SemaphoreType.DMA((2 * PLANES,)),
            pltpu.SemaphoreType.DMA,
            pltpu.SemaphoreType.DMA((PLANES,)),
        ],
        compiler_params=pltpu.CompilerParams(collective_id=0, has_side_effects=True),
    )(fact_keys.reshape(2, 128), dim_keys.reshape(BLOCK // 128, 128), dim_payload)


def solution(mesh):
    return jax.shard_map(
        on_device,
        mesh=mesh,
        in_specs=(P(("row", "col")), P(("row", "col")), P(("row", "col"), None)),
        out_specs=P(("row", "col"), None),
        check_vma=False,
    )
```
